16 devices in a mesh: data: 16 (over z, y, x, core).
Axes of the slice: x: 2, y: 2, z: 2, core: 2. Of those that a mesh axis runs over, the one named last changes fastest.
Arguments:
- grad_attn: bfloat16 [16, 12, 589824], P('data')
- grad_mlp: bfloat16 [16, 6, 2359296], P('data')
- grad_wide: bfloat16 [16, 3, 3072], P('data')
- grad_vec: bfloat16 [16, 29, 768], P('data')
- weight_attn: float32 [12, 589824], P(None, 'data')
- weight_mlp: float32 [6, 2359296], P(None, 'data')
- weight_wide: float32 [3, 3072], P(None, 'data')
- weight_vec: float32 [29, 768], P(None, 'data')
- mom1_attn: float32 [12, 589824], P(None, 'data')
- mom1_mlp: float32 [6, 2359296], P(None, 'data')
- mom1_wide: float32 [3, 3072], P(None, 'data')
- mom1_vec: float32 [29, 768], P(None, 'data')
- mom2_attn: float32 [12, 589824], P(None, 'data')
- mom2_mlp: float32 [6, 2359296], P(None, 'data')
- mom2_wide: float32 [3, 3072], P(None, 'data')
- mom2_vec: float32 [29, 768], P(None, 'data')
Outputs:
- output 1: bfloat16 [12, 589824], replicated
- output 2: bfloat16 [6, 2359296], replicated
- output 3: bfloat16 [3, 3072], replicated
- output 4: bfloat16 [29, 768], replicated
- output 5: float32 [12, 589824], P(None, 'data')
- output 6: float32 [6, 2359296], P(None, 'data')
- output 7: float32 [3, 3072], P(None, 'data')
- output 8: float32 [29, 768], P(None, 'data')
- output 9: float32 [12, 589824], P(None, 'data')
- output 10: float32 [6, 2359296], P(None, 'data')
- output 11: float32 [3, 3072], P(None, 'data')
- output 12: float32 [29, 768], P(None, 'data')
- output 13: float32 [12, 589824], P(None, 'data')
- output 14: float32 [6, 2359296], P(None, 'data')
- output 15: float32 [3, 3072], P(None, 'data')
- output 16: float32 [29, 768], P(None, 'data')
All inputs are finite; a program needn't handle non-finite values.
Results may differ from the reference program's by a relative error of at most 0.001.
Values are sent between devices in bfloat16 or wider.
A program may use at most 1 GiB of HBM per device.

```python
import jax
import jax.numpy as jnp

GROUP_SIZE = 16
LAYERS = 3
D = 768
FF = 3072
STEP_NUMBER = 10

LEARN_RATE = 0.04
BETA_FIRST = 0.9
BETA_SECOND = 0.999
EPSILON = 1e-6
WEIGHT_DECAY = 0.01
MAX_NORM = 1.0
TARGET_NORM = 3.0


def bank_layout():
    gain_rows = jnp.array([1.0, 0.0, 0.0, 0.0, 0.0, 0.0, 1.0, 0.0, 0.0] * LAYERS + [1.0, 0.0])
    counts = (4 * LAYERS, 2 * LAYERS, LAYERS, 9 * LAYERS + 2)
    lengths = (D * D, D * FF, FF, D)
    base_scales = (
        jnp.full((4 * LAYERS,), D ** -0.5),
        jnp.array([D ** -0.5, FF ** -0.5] * LAYERS),
        jnp.full((LAYERS,), 0.05),
        0.05 + 0.15 * gain_rows,
    )
    offsets = (jnp.zeros((4 * LAYERS,)), jnp.zeros((2 * LAYERS,)), jnp.zeros((LAYERS,)), gain_rows)
    return counts, lengths, base_scales, offsets


def setup_inputs(seed: int = 0) -> dict:
    root_key = jax.random.key(seed)
    counts, lengths, base_scales, offsets = bank_layout()
    bank_keys = [jax.random.split(jax.random.fold_in(root_key, bank_index), 6) for bank_index in range(4)]
    grad_mults = [jnp.exp(jax.random.uniform(bank_keys[bank_index][0], (counts[bank_index],), minval=-1.0, maxval=1.0)) for bank_index in range(4)]
    weighted = sum(lengths[bank_index] * jnp.sum(grad_mults[bank_index] ** 2) for bank_index in range(4))
    grad_unit = TARGET_NORM * jnp.sqrt(GROUP_SIZE / weighted)
    clip_guess = MAX_NORM / TARGET_NORM
    grad_banks, weights, firsts, seconds = [], [], [], []
    for bank_index in range(4):
        bank_keyset = bank_keys[bank_index]
        row_count = counts[bank_index]
        row_length = lengths[bank_index]
        grad_scale = grad_unit * grad_mults[bank_index]
        device_grads = jax.random.normal(bank_keyset[1], (GROUP_SIZE, row_count, row_length)) * grad_scale[None, :, None]
        grad_banks.append(device_grads.astype(jnp.bfloat16))
        weight_spread = jnp.exp(jax.random.uniform(bank_keyset[2], (row_count,), minval=-1.2, maxval=1.2))
        row_scale = base_scales[bank_index] * weight_spread
        weights.append(offsets[bank_index][:, None] + row_scale[:, None] * jax.random.normal(bank_keyset[3], (row_count, row_length)))
        moment_unit = clip_guess * grad_scale / GROUP_SIZE ** 0.5
        firsts.append(0.1 * moment_unit[:, None] * jax.random.normal(bank_keyset[4], (row_count, row_length)))
        seconds.append(0.001 * (moment_unit * moment_unit)[:, None] * jnp.exp(0.5 * jax.random.normal(bank_keyset[5], (row_count, row_length))))
    bank_names = ("attn", "mlp", "wide", "vec")
    inputs = {}
    for prefix, arrays in (("grad_", grad_banks), ("weight_", weights), ("mom1_", firsts), ("mom2_", seconds)):
        for bank_index in range(4):
            inputs[prefix + bank_names[bank_index]] = arrays[bank_index]
    return inputs


def lamb_bank(mean_grad, weight, first_moment, second_moment, clip_coef):
    clipped = clip_coef * mean_grad
    new_first = BETA_FIRST * first_moment + (1.0 - BETA_FIRST) * clipped
    new_second = BETA_SECOND * second_moment + (1.0 - BETA_SECOND) * (clipped * clipped)
    update = (new_first / (1.0 - BETA_FIRST ** STEP_NUMBER)) / (jnp.sqrt(new_second / (1.0 - BETA_SECOND ** STEP_NUMBER)) + EPSILON) + WEIGHT_DECAY * weight
    weight_norm = jnp.sqrt(jnp.sum(weight * weight, axis=1, keepdims=True))
    update_norm = jnp.sqrt(jnp.sum(update * update, axis=1, keepdims=True))
    new_weight = weight - LEARN_RATE * (weight_norm / update_norm) * update
    return new_weight.astype(jnp.bfloat16), new_weight, new_first, new_second


def reference(grad_attn, grad_mlp, grad_wide, grad_vec, weight_attn, weight_mlp, weight_wide, weight_vec, mom1_attn, mom1_mlp, mom1_wide, mom1_vec, mom2_attn, mom2_mlp, mom2_wide, mom2_vec):
    mean_attn = jnp.sum(grad_attn, axis=0, dtype=jnp.float32) / GROUP_SIZE
    mean_mlp = jnp.sum(grad_mlp, axis=0, dtype=jnp.float32) / GROUP_SIZE
    mean_wide = jnp.sum(grad_wide, axis=0, dtype=jnp.float32) / GROUP_SIZE
    mean_vec = jnp.sum(grad_vec, axis=0, dtype=jnp.float32) / GROUP_SIZE
    total_square = jnp.sum(mean_attn * mean_attn) + jnp.sum(mean_mlp * mean_mlp) + jnp.sum(mean_wide * mean_wide) + jnp.sum(mean_vec * mean_vec)
    clip_coef = jnp.minimum(1.0, MAX_NORM / jnp.sqrt(total_square))
    attn_out = lamb_bank(mean_attn, weight_attn, mom1_attn, mom2_attn, clip_coef)
    mlp_out = lamb_bank(mean_mlp, weight_mlp, mom1_mlp, mom2_mlp, clip_coef)
    wide_out = lamb_bank(mean_wide, weight_wide, mom1_wide, mom2_wide, clip_coef)
    vec_out = lamb_bank(mean_vec, weight_vec, mom1_vec, mom2_vec, clip_coef)
    return (attn_out[0], mlp_out[0], wide_out[0], vec_out[0], attn_out[1], mlp_out[1], wide_out[1], vec_out[1], attn_out[2], mlp_out[2], wide_out[2], vec_out[2], attn_out[3], mlp_out[3], wide_out[3], vec_out[3])
```

```python
import functools

import jax
import jax.numpy as jnp
from jax import lax
from jax.experimental import pallas as pl
from jax.experimental.pallas import tpu as pltpu
from jax.sharding import PartitionSpec as P

STEP_NUMBER = 10
LEARN_RATE = 0.04
BETA_FIRST = 0.9
BETA_SECOND = 0.999
EPSILON = 1e-6
WEIGHT_DECAY = 0.01
MAX_NORM = 1.0
FIRST_SCALE = 1.0 / (1.0 - BETA_FIRST ** STEP_NUMBER)
SECOND_SCALE = 1.0 / (1.0 - BETA_SECOND ** STEP_NUMBER)

MESH = pl.DeviceIdType.MESH
F32 = jnp.float32
BF16 = jnp.bfloat16
DEVICES = 16
LANES = 128
KT = 48
CHUNK = 3 * KT * LANES
ATTN_COLS = 2 * KT * LANES
MLP_COLS = 4 * KT * LANES
ATTN_W = 3 * ATTN_COLS
MLP_W = 6 * MLP_COLS
STEP = 4 * LANES
STEPS = KT * LANES // STEP
TILE = 8
A_ROWS = 12
M_ROWS = 6
GROUPS = 3
PARTS = 3
HALF = LANES // 2
VMEM_LIMIT = 67043328
SMALL = (32, 128)
WEIGHT = (1, 2, 4)
BLOCKS = [slice(row, row + TILE) for row in range(0, SMALL[0], TILE)]
ORDER = [(g, j) for j in range(3) for g in range(3)]
AXES = ((0, 1, 2), (1, 2, 0), (2, 0, 1))


def position():
    me = lax.axis_index("data")
    bits = [lax.rem(me // 2, 2), lax.rem(me // 4, 2), lax.rem(me // 8, 2)]
    return me, lax.rem(me, 2), bits


def flip(bit, by):
    return bit + by - 2 * bit * by


def chip_at(bits, flips):
    total = 0
    for axis in range(3):
        total = total + flip(bits[axis], flips[axis]) * WEIGHT[axis]
    return total


def flips_of(group, first, second, third):
    flips = [0, 0, 0]
    for axis, by in zip(AXES[group], (first, second, third)):
        flips[axis] = by
    return flips


def columns(group, part, owner):
    if part == 0:
        start = owner * ATTN_W + group * ATTN_COLS
        return pl.ds(pl.multiple_of(start, ATTN_COLS), ATTN_COLS)
    start = owner * MLP_W + group * 2 * MLP_COLS + (part - 1) * MLP_COLS
    return pl.ds(pl.multiple_of(start, MLP_COLS), MLP_COLS)


def signal_all(me):
    barrier = pltpu.get_barrier_semaphore()

    @pl.loop(1, DEVICES)
    def _(t):
        pl.semaphore_signal(barrier, inc=1, device_id=(lax.rem(me + t, DEVICES),), device_id_type=MESH)

    pl.semaphore_wait(barrier, DEVICES - 1)


def spread(me, source, slots, send_sem, recv_sem):
    def copy(t):
        peer = lax.rem(me + t, DEVICES)
        return pltpu.make_async_remote_copy(
            src_ref=source(peer), dst_ref=slots.at[me], send_sem=send_sem.at[t], recv_sem=recv_sem.at[me],
            device_id=(peer,), device_id_type=MESH)

    @pl.loop(1, DEVICES)
    def _(t):
        copy(t).start()


def gather_wait(me, source, slots, send_sem, recv_sem):
    @pl.loop(1, DEVICES)
    def _(t):
        peer = lax.rem(me + t, DEVICES)
        pltpu.make_async_remote_copy(
            src_ref=source(peer), dst_ref=slots.at[peer], send_sem=send_sem.at[t], recv_sem=recv_sem.at[peer],
            device_id=(peer,), device_id_type=MESH).wait()


def put_cols(ref, lo, step, value):
    ref[:, pl.ds(pl.multiple_of(lo * LANES + step * STEP, STEP), STEP)] = value


def pack_rows(part, load, put):
    if part == 0:
        a, b = load(0), load(KT)
        put(0, a[0:8])
        put(KT, b[0:8])
        put(2 * KT, jnp.concatenate([a[8:12], b[8:12]], axis=0))
    else:
        d = load(3 * KT)
        for t in range(3):
            put(t * KT, jnp.concatenate([load(t * KT), d[2 * t:2 * t + 2]], axis=0))


def pack_sum(part, own, partner, out, extra):
    @pl.loop(0, STEPS)
    def _(step):
        def cols(lo):
            return pl.ds(pl.multiple_of(lo * LANES + step * STEP, STEP), STEP)

        def put(lo, value):
            if extra is not None:
                value = value + extra[:, cols(lo)]
            put_cols(out, lo, step, value)

        pack_rows(part, lambda lo: own[:, cols(lo)].astype(F32) + partner[:, cols(lo)].astype(F32), put)


def fold(x):
    return sum(x[:, l:l + LANES] for l in range(0, x.shape[1], LANES))


def reduce_kernel(ga, gm, gsmall, pa, pm, gs_a, gs_m, small_out, clip_out,
                  sbuf, r1, r2, r3, raw_a, raw_m, small_slots, norm_slots, acc,
                  d_send, d_recv, s1, q1, s2, q2, s3, q3, load_sem, out_sem, t_send, t_recv, n_send, n_recv):
    me, core, bits = position()
    partner = me + 1 - 2 * core
    signal_all(me)

    def neighbour(axis):
        return me + (2, 4, 8)[axis] * (1 - 2 * bits[axis])


    def owner_chip(half, i, g):
        return chip_at(bits, flips_of(g, 1 - half, 1 - i // 2, 1 - lax.rem(i, 2)))

    def pair_copy(half, i, g, j):
        chip = owner_chip(half, i, g)
        src = (ga, gm)[j > 0].at[0, :, columns(g, j, 2 * chip + 1 - core)]
        dst = (pa, pm)[j > 0].at[:, columns(g, j, chip)]
        return pltpu.make_async_remote_copy(
            src_ref=src, dst_ref=dst, send_sem=d_send.at[half, i, g, j], recv_sem=d_recv.at[half, i, g, j],
            device_id=(partner,), device_id_type=MESH)

    for half in range(2):
        @pl.loop(0, 4)
        def _(i):
            for g, j in ORDER:
                pair_copy(half, i, g, j).start()
        if half == 0:
            spread(me, lambda peer: gsmall.at[peer], small_slots, t_send, t_recv)

    def loads(half, i, g, j, slot):
        chip = owner_chip(half, i, g)
        buf = (raw_a, raw_m)[j > 0]
        own = pltpu.make_async_copy((ga, gm)[j > 0].at[0, :, columns(g, j, 2 * chip + core)], buf.at[slot, 0], load_sem.at[slot, 0])
        par = pltpu.make_async_copy((pa, pm)[j > 0].at[:, columns(g, j, chip)], buf.at[slot, 1], load_sem.at[slot, 1])
        return own, par

    def start_loads(half, i, g, j, slot):
        own, par = loads(half, i, g, j, slot)
        own.start()
        pair_copy(half, i, g, j).wait_recv()
        par.start()

    def send(axis, src, dst, ss, rs):
        return pltpu.make_async_remote_copy(src_ref=src, dst_ref=dst, send_sem=ss, recv_sem=rs,
                                            device_id=(neighbour(axis),), device_id_type=MESH)

    def send1(i, g, j):
        return send(AXES[g][0], sbuf.at[g, i, j], r1.at[g, i, j], s1.at[g, i, j], q1.at[g, i, j])

    def send2(i, g, j):
        return send(AXES[g][1], r1.at[g, i, j], r2.at[g, i, j], s2.at[g, i, j], q2.at[g, i, j])

    def send3(g, j):
        return send(AXES[g][2], r2.at[g, 0, j], r3.at[g, j], s3.at[g, j], q3.at[g, j])

    def sweep(half, i, use):
        start_loads(half, i, *ORDER[0], 0)
        for n, (g, j) in enumerate(ORDER):
            if n + 1 < len(ORDER):
                start_loads(half, i, *ORDER[n + 1], (n + 1) % 2)
            for copy in loads(half, i, g, j, n % 2):
                copy.wait()
            buf = (raw_a, raw_m)[j > 0]
            use(i, g, j, buf.at[n % 2, 0], buf.at[n % 2, 1])

    def first(i, g, j, own, par):
        pack_sum(j, own, par, sbuf.at[g, i, j], None)
        send1(i, g, j).start()

    @pl.loop(0, 4)
    def _(i):
        sweep(0, i, first)

    def second(i, g, j, own, par):
        send1(i, g, j).wait_recv()
        pack_sum(j, own, par, r1.at[g, i, j], r1.at[g, i, j])

    def second_send(i, g, j, own, par):
        second(i, g, j, own, par)
        send2(i, g, j).start()

    @pl.loop(0, 2)
    def _(i):
        sweep(1, i, second_send)

    @pl.loop(2, 4)
    def _(i):
        sweep(1, i, second)

    def add_into(dst, src):
        @pl.loop(0, CHUNK // STEP // 2)
        def _(step):
            cols = pl.ds(pl.multiple_of(step * STEP * 2, STEP * 2), STEP * 2)
            dst[:, cols] = dst[:, cols] + src[:, cols]

    for i in range(2):
        for g, j in ORDER:
            send2(i, g, j).wait_recv()
            add_into(r2.at[g, i, j], r1.at[g, 2 + i, j])
            if i == 0:
                send3(g, j).start()

    gather_wait(me, lambda peer: gsmall.at[peer], small_slots, t_send, t_recv)
    small_slots[me] = gsmall[me]
    small = jnp.zeros(SMALL, F32)
    for slot in range(DEVICES):
        small = small + small_slots[slot].astype(F32)
    small = small * (1.0 / DEVICES)
    small_out[...] = small
    sq = small * small
    acc[...] = sum(sq[rows] for rows in BLOCKS)

    def out_copies(g, j):
        return [pltpu.make_async_copy(r3.at[(g, j) + src], (gs_a, gs_m)[j > 0].at[dst], out_sem.at[g, j, n])
                for n, (src, dst) in enumerate(unpack_moves(g, j, 0))]

    for g, j in ORDER:
        send3(g, j).wait_recv()

        def body(step, sums):
            cols = pl.ds(pl.multiple_of(step * STEP * 2, STEP * 2), STEP * 2)
            value = (r3[g, j, :, cols] + r2[g, 1, j, :, cols]) * (1.0 / DEVICES)
            r3[g, j, :, cols] = value
            return sums + value * value

        sums = lax.fori_loop(0, CHUNK // STEP // 2, body, jnp.zeros((TILE, STEP * 2), F32))
        acc[...] += fold(sums)
        for copy in out_copies(g, j):
            copy.start()

    norm_slots[me] = acc[...]
    spread(me, lambda peer: acc, norm_slots, n_send, n_recv)
    gather_wait(me, lambda peer: acc, norm_slots, n_send, n_recv)
    total = jnp.sum(sum(norm_slots[slot] for slot in range(DEVICES)), axis=(0, 1), keepdims=True)
    clip_out[...] = jnp.broadcast_to(jnp.minimum(1.0, MAX_NORM / jnp.sqrt(total)), (TILE, LANES))

    for g, j in ORDER:
        for copy in out_copies(g, j):
            copy.wait()
        send3(g, j).wait_send()
        for i in range(2):
            send2(i, g, j).wait_send()

    @pl.loop(0, 4)
    def _(i):
        for g, j in ORDER:
            send1(i, g, j).wait_send()
            pair_copy(0, i, g, j).wait_send()
            pair_copy(1, i, g, j).wait_send()


def reduce_call(ga, gm, gsmall):
    hbm = pl.BlockSpec(memory_space=pl.ANY)
    vmem = pl.BlockSpec(memory_space=pltpu.VMEM)
    dma = pltpu.SemaphoreType.DMA
    outs = pl.pallas_call(
        reduce_kernel,
        out_shape=[
            jax.ShapeDtypeStruct((A_ROWS, 8 * ATTN_W), BF16),
            jax.ShapeDtypeStruct((M_ROWS, 8 * MLP_W), BF16),
            jax.ShapeDtypeStruct((A_ROWS, ATTN_W), F32),
            jax.ShapeDtypeStruct((M_ROWS, MLP_W), F32),
            jax.ShapeDtypeStruct(SMALL, F32),
            jax.ShapeDtypeStruct((TILE, LANES), F32),
        ],
        in_specs=[hbm, hbm, vmem],
        out_specs=[hbm] * 4 + [vmem] * 2,
        scratch_shapes=[
            pltpu.VMEM((GROUPS, 4, PARTS, TILE, CHUNK), F32),
            pltpu.VMEM((GROUPS, 4, PARTS, TILE, CHUNK), F32),
            pltpu.VMEM((GROUPS, 2, PARTS, TILE, CHUNK), F32),
            pltpu.VMEM((GROUPS, PARTS, TILE, CHUNK), F32),
            pltpu.VMEM((2, 2, A_ROWS, ATTN_COLS), BF16),
            pltpu.VMEM((2, 2, M_ROWS, MLP_COLS), BF16),
            pltpu.VMEM((DEVICES,) + SMALL, BF16),
            pltpu.VMEM((DEVICES, TILE, LANES), F32),
            pltpu.VMEM((TILE, LANES), F32),
            dma((2, 4, GROUPS, PARTS)), dma((2, 4, GROUPS, PARTS)),
            dma((GROUPS, 4, PARTS)), dma((GROUPS, 4, PARTS)),
            dma((GROUPS, 2, PARTS)), dma((GROUPS, 2, PARTS)),
            dma((GROUPS, PARTS)), dma((GROUPS, PARTS)),
            dma((2, 2)), dma((GROUPS, PARTS, 5)),
            dma((DEVICES,)), dma((DEVICES,)), dma((DEVICES,)), dma((DEVICES,)),
        ],
        compiler_params=pltpu.CompilerParams(collective_id=0, has_side_effects=True, vmem_limit_bytes=VMEM_LIMIT),
        name="reduce_scatter",
    )(ga, gm, gsmall)
    return outs[2:]


def moments(g, m, v, clip):
    return (BETA_FIRST * m + ((1.0 - BETA_FIRST) * clip) * g,
            BETA_SECOND * v + ((1.0 - BETA_SECOND) * (clip * clip)) * (g * g))


def direction(w, new_m, new_v):
    return (new_m * FIRST_SCALE) / (jnp.sqrt(new_v * SECOND_SCALE) + EPSILON) + WEIGHT_DECAY * w


def chunk_columns(g, j):
    n, width = (g, ATTN_COLS) if j == 0 else (2 * g + j - 1, MLP_COLS)
    return n, pl.ds(n * width, width)


def wide_pieces(ref):
    return [ref[rows.start:rows.start + GROUPS, HALF:] for rows in BLOCKS[:GROUPS]]


def update_kernel(*refs):
    banks, (clip, gs_s), vec, wide = (refs[:4], refs[4:8]), refs[8:10], refs[10:13], refs[13:16]
    outs = refs[16:18], refs[18:20]
    small_outs, u_s, w_s, sums = (refs[20:22], refs[22:24]), refs[24], refs[25], (refs[26:28], refs[28:30])
    bufs, load_sem, out_sem = refs[30:32], refs[32], refs[33]

    def loads(g, j):
        n, cols = chunk_columns(g, j)
        return [pltpu.make_async_copy(ref.at[:, cols], bufs[j > 0].at[n, k], load_sem.at[g, j, k]) for k, ref in enumerate(banks[j > 0])]

    def stores(g, j):
        n, cols = chunk_columns(g, j)
        return [pltpu.make_async_copy(bufs[j > 0].at[n, 2 + k], ref.at[:, cols], out_sem.at[g, j, k]) for k, ref in enumerate(outs[j > 0])]

    for g, j in ORDER:
        for copy in loads(g, j):
            copy.start()

    c = clip[0:1, 0:1]
    u_s[...] = jnp.zeros(SMALL, F32)
    w_s[...] = jnp.zeros(SMALL, F32)
    grads = gs_s[0:vec[0].shape[0], 0:vec[0].shape[1]], jnp.concatenate(wide_pieces(gs_s), axis=1)
    for k, (grad, (w, m, v)) in enumerate(zip(grads, (vec, wide))):
        w = w[...]
        new = moments(grad, m[...], v[...], c)
        for ref, value in zip(small_outs[k], new):
            ref[...] = value
        for ref, value in ((u_s, direction(w, *new)), (w_s, w)):
            if k == 0:
                ref[0:value.shape[0], 0:value.shape[1]] = value
            else:
                for t, rows in enumerate(BLOCKS[:GROUPS]):
                    ref[rows.start:rows.start + GROUPS, HALF:] = value[:, t * HALF:(t + 1) * HALF]

    totals = [[jnp.zeros((rows, LANES), F32)] * 2 for rows in (A_ROWS, M_ROWS)]
    for g, j in ORDER:
        for copy in loads(g, j):
            copy.wait()
        buf, n = bufs[j > 0], chunk_columns(g, j)[0]
        width = STEP * (1 + (j > 0))

        def body(step, total):
            cols = pl.ds(pl.multiple_of(step * width, width), width)
            grad, w, m, v = (buf[n, k, :, cols] for k in range(4))
            new = moments(grad, m, v, c)
            for k in range(2):
                buf[n, 2 + k, :, cols] = new[k]
            return tuple(x + fold(y * y) for x, y in zip(total, (direction(w, *new), w)))

        totals[j > 0] = lax.fori_loop(0, buf.shape[3] // width, body, tuple(totals[j > 0]))
        for copy in stores(g, j):
            copy.start()
    for pair, total in zip(sums, totals):
        for ref, value in zip(pair, total):
            ref[...] = value
    for g, j in ORDER:
        for copy in stores(g, j):
            copy.wait()


def update_call(attn, mlp, *small):
    def whole(shape):
        return pl.BlockSpec(shape, lambda n: (0, 0))

    hbm = pl.BlockSpec(memory_space=pl.ANY)
    outs = [small[2].shape] * 2 + [small[5].shape] * 2 + [SMALL] * 2 + [(A_ROWS, LANES)] * 2 + [(M_ROWS, LANES)] * 2
    return pl.pallas_call(
        update_kernel,
        grid=(1,),
        in_specs=[hbm] * 8 + [whole(x.shape) for x in small],
        out_specs=[hbm] * 4 + [whole(shape) for shape in outs],
        out_shape=[jax.ShapeDtypeStruct(shape, F32) for shape in [(A_ROWS, ATTN_W)] * 2 + [(M_ROWS, MLP_W)] * 2 + outs],
        scratch_shapes=[
            pltpu.VMEM((GROUPS, 4, A_ROWS, ATTN_COLS), F32),
            pltpu.VMEM((2 * GROUPS, 4, M_ROWS, MLP_COLS), F32),
            pltpu.SemaphoreType.DMA((GROUPS, PARTS, 4)),
            pltpu.SemaphoreType.DMA((GROUPS, PARTS, 2)),
        ],
        compiler_params=pltpu.CompilerParams(vmem_limit_bytes=VMEM_LIMIT),
        name="update",
    )(*attn, *mlp, *small)


def gather_kernel(*rest):
    banks, rest = (rest[:3], rest[3:6]), rest[6:]
    stats, (full, small_full, nw_a, nw_m, nw_s) = rest[:6], rest[6:11]
    stat_bufs, rest = rest[11:17], rest[17:]
    (sbuf, st_a, st_m, tile, slots, small_buf, x_send, x_recv, d_send, d_recv,
     own_sem, new_sem, load_sem, stat_sem, n_send, n_recv, t_send, t_recv) = rest
    u_s, w_s, uu_a, ww_a, uu_m, ww_m = stat_bufs
    me, core, bits = position()
    partner = me + 1 - 2 * core
    stat_copies = [pltpu.make_async_copy(src, dst, stat_sem.at[n]) for n, (src, dst) in enumerate(zip(stats, stat_bufs))]
    for copy in stat_copies:
        copy.start()
    signal_all(me)

    def chunk(g, j):
        return (st_a, st_m)[j > 0], *chunk_columns(g, j)

    def loads(g, j):
        buf, n, cols = chunk(g, j)
        return [pltpu.make_async_copy(ref.at[:, cols], buf.at[n, k], load_sem.at[g, j, k]) for k, ref in enumerate(banks[j > 0])]

    for copy in stat_copies:
        copy.wait()
    for g, j in ORDER:
        for copy in loads(g, j):
            copy.start()

    lane = lax.broadcasted_iota(jnp.int32, (TILE, LANES), 1)
    out = jnp.zeros((TILE, LANES), F32)

    def pad8(x):
        return jnp.concatenate([x, jnp.zeros((8 - x.shape[0], x.shape[1]), F32)], axis=0)

    for k, (a, m, s) in enumerate([(uu_a, uu_m, u_s), (ww_a, ww_m, w_s)]):
        a, m, s = a[...], m[...], s[...] * s[...]
        vec = jnp.where(lax.broadcasted_iota(jnp.int32, SMALL, 1) < HALF, s, 0.0)
        wide = s - vec
        blocks = [a[0:TILE], pad8(a[TILE:]), pad8(m)] + [vec[rows] for rows in BLOCKS] + [sum(wide[rows] for rows in BLOCKS)]
        for l, block in enumerate(blocks):
            out = jnp.where(lane == TILE * k + l, jnp.sum(block, axis=1, keepdims=True), out)
    tile[...] = out
    slots[me] = out
    spread(me, lambda peer: tile, slots, n_send, n_recv)
    gather_wait(me, lambda peer: tile, slots, n_send, n_recv)
    root = jnp.sqrt(sum(slots[slot] for slot in range(DEVICES)))
    ratio = [LEARN_RATE * (root[:, 8 + l:9 + l] / root[:, l:l + 1]) for l in range(8)]

    def place(g, r, j):
        owner = 2 * chip_at(bits, flips_of(g, lax.rem(r, 2), lax.rem(r // 2, 2), r // 4)) + core
        return full.at[owner, g, j]

    def copy_to(g, r, j, to, arrived, sends, recvs, src):
        return pltpu.make_async_remote_copy(
            src_ref=src, dst_ref=place(g, r, j), send_sem=sends.at[g, arrived, j], recv_sem=recvs.at[g, arrived, j],
            device_id=(to,), device_id_type=MESH)

    def forward(g, r, j, step, src=None):
        axis = AXES[g][step]
        to = me + WEIGHT[axis] * 2 * (1 - 2 * bits[axis])
        copy_to(g, r, j, to, r + WEIGHT[step], x_send, x_recv, place(g, r, j) if src is None else src).start()

    def to_partner(g, r, j, src=None):
        return copy_to(g, r, j, partner, r, d_send, d_recv, place(g, r, j) if src is None else src)

    def arrival(g, r, j):
        return copy_to(g, r, j, partner, r, x_send, x_recv, place(g, r, j))

    def own_copy(g, j):
        return pltpu.make_async_copy(sbuf.at[g, j], place(g, 0, j), own_sem.at[g, j])

    def new_copy(g, j):
        buf, n, cols = chunk(g, j)
        return pltpu.make_async_copy(buf.at[n, 0], (nw_a, nw_m)[j > 0].at[:, cols], new_sem.at[g, j])

    for g, j in ORDER:
        for copy in loads(g, j):
            copy.wait()
        buf, n, _ = chunk(g, j)
        scale = jnp.concatenate([ratio[0], ratio[1][0:4]], axis=0) if j == 0 else ratio[2][0:6]

        @pl.loop(0, STEPS)
        def _(step):
            def new(lo):
                cols = pl.ds(pl.multiple_of(lo * LANES + step * STEP, STEP), STEP)
                w, m, v = (buf[n, k, :, cols] for k in range(3))
                value = w - scale * direction(w, m, v)
                buf[n, 0, :, cols] = value
                return value

            pack_rows(j, new, lambda lo, value: put_cols(sbuf.at[g, j], lo, step, value.astype(BF16)))

        forward(g, 0, j, 0, sbuf.at[g, j])
        own_copy(g, j).start()
        new_copy(g, j).start()

    for step in (1, 2):
        for g, j in ORDER:
            forward(g, 0, j, step, sbuf.at[g, j])
    for g, j in ORDER:
        to_partner(g, 0, j, sbuf.at[g, j]).start()
    for rows, scale in zip(BLOCKS, ratio[3:]):
        nw_s[rows] = w_s[rows] - jnp.where(lane < HALF, scale, ratio[7]) * u_s[rows]
    small_buf[...] = nw_s[...].astype(BF16)
    spread(me, lambda peer: small_buf, small_full, t_send, t_recv)

    def receive(r, steps):
        for g, j in ORDER:
            arrival(g, r, j).wait_recv()
            for step in steps:
                forward(g, r, j, step)
            to_partner(g, r, j).start()

    receive(1, (1, 2))

    @pl.loop(2, 4)
    def _(r):
        receive(r, (2,))

    @pl.loop(4, 8)
    def _(r):
        receive(r, ())

    gather_wait(me, lambda peer: small_buf, small_full, t_send, t_recv)
    small_full[me] = small_buf[...]
    for g, j in ORDER:
        own_copy(g, j).wait()
        new_copy(g, j).wait()

    @pl.loop(0, 8)
    def _(r):
        for g, j in ORDER:
            to_partner(g, r, j).wait()

    @pl.loop(1, 8)
    def _(r):
        for g, j in ORDER:
            arrival(g, r, j).wait_send()


def gather_call(*args):
    hbm = pl.BlockSpec(memory_space=pl.ANY)
    vmem = pl.BlockSpec(memory_space=pltpu.VMEM)
    dma = pltpu.SemaphoreType.DMA
    sems = [dma((3, 8, 3))] * 4 + [dma((GROUPS, PARTS))] * 2 + [dma((3, 3, 3)), dma((6,))] + [dma((DEVICES,))] * 4
    return pl.pallas_call(
        gather_kernel,
        out_shape=[
            jax.ShapeDtypeStruct((DEVICES, GROUPS, PARTS, TILE, CHUNK), BF16),
            jax.ShapeDtypeStruct((DEVICES,) + SMALL, BF16),
            jax.ShapeDtypeStruct((A_ROWS, ATTN_W), F32),
            jax.ShapeDtypeStruct((M_ROWS, MLP_W), F32),
            jax.ShapeDtypeStruct(SMALL, F32),
        ],
        in_specs=[hbm] * len(args),
        out_specs=[hbm, vmem, hbm, hbm, vmem],
        scratch_shapes=[pltpu.VMEM(x.shape, F32) for x in args[6:]] + [
            pltpu.VMEM((GROUPS, PARTS, TILE, CHUNK), BF16),
            pltpu.VMEM((3, 3, A_ROWS, ATTN_COLS), F32),
            pltpu.VMEM((M_ROWS, 3, M_ROWS, MLP_COLS), F32),
            pltpu.VMEM((TILE, LANES), F32),
            pltpu.VMEM((DEVICES, TILE, LANES), F32),
            pltpu.VMEM(SMALL, BF16),
        ] + sems,
        compiler_params=pltpu.CompilerParams(collective_id=1, has_side_effects=True, vmem_limit_bytes=VMEM_LIMIT),
        name="all_gather",
    )(*args)


def unpack_moves(g, j, owner):
    if j == 0:
        start = owner * ATTN_W + g * ATTN_COLS
        moves = [(0, 8, 0, 2, 0, 0)] + [(4 * t, 4, 2, 1, 8, t) for t in range(2)]
    else:
        start = owner * MLP_W + (2 * g + j - 1) * MLP_COLS
        moves = [(0, 4, 0, 3, 0, 0), (4, 2, 0, 3, 4, 0)] + [(M_ROWS, 2, t, 1, 2 * t, 3) for t in range(3)]
    third = KT * LANES
    for row, rows, lo, width, to, at in moves:
        cols = pl.ds(pl.multiple_of(start + at * third, third), width * third)
        yield (pl.ds(row, rows), pl.ds(lo * third, width * third)), (pl.ds(to, rows), cols)


def unpack_kernel(full, small_full, nw_s, rep_a, rep_m, rep_vec, rep_wide, nw_vec, nw_wide, buf, load_sem, out_sem):
    sets = buf.shape[0]

    def loads(owner):
        return [pltpu.make_async_copy(full.at[owner, g, j], buf.at[lax.rem(owner, sets), g, j], load_sem.at[lax.rem(owner, sets), g, j]) for g, j in ORDER]

    def outs(owner, g, j):
        slot = lax.rem(owner, sets)
        rep = (rep_a, rep_m)[j > 0]
        return [pltpu.make_async_copy(buf.at[(slot, g, j) + src], rep.at[dst], out_sem.at[slot, g, j, n])
                for n, (src, dst) in enumerate(unpack_moves(g, j, owner))]

    def drain(owner):
        for g, j in ORDER:
            for copy in outs(owner, g, j):
                copy.wait()

    for owner in range(2):
        for copy in loads(owner):
            copy.start()

    @pl.loop(0, DEVICES)
    def _(owner):
        @pl.when(owner >= 2)
        def _():
            drain(owner - 2)

        @pl.when(owner < DEVICES - 2)
        def _():
            for copy in loads(owner + 2):
                copy.start()

        for (g, j), copy in zip(ORDER, loads(owner)):
            copy.wait()
            for move in outs(owner, g, j):
                move.start()

    vec = nw_vec.shape
    nw_vec[...] = nw_s[0:vec[0], 0:vec[1]]
    nw_wide[...] = jnp.concatenate(wide_pieces(nw_s), axis=1)
    shares = [small_full[n].astype(F32) for n in range(DEVICES)]
    rep_vec[...] = jnp.concatenate([x[0:vec[0], 0:vec[1]] for x in shares], axis=1).astype(BF16)
    rep_wide[...] = jnp.concatenate([piece for x in shares for piece in wide_pieces(x)], axis=1).astype(BF16)
    for owner in (DEVICES - 2, DEVICES - 1):
        drain(owner)


def unpack_call(full, small_full, nw_s):
    hbm = pl.BlockSpec(memory_space=pl.ANY)
    vmem = pl.BlockSpec(memory_space=pltpu.VMEM)
    return pl.pallas_call(
        unpack_kernel,
        in_specs=[hbm, vmem, vmem],
        out_specs=[hbm] * 2 + [vmem] * 4,
        out_shape=[
            jax.ShapeDtypeStruct((A_ROWS, DEVICES * ATTN_W), BF16),
            jax.ShapeDtypeStruct((M_ROWS, DEVICES * MLP_W), BF16),
            jax.ShapeDtypeStruct((29, 768), BF16),
            jax.ShapeDtypeStruct((3, 3072), BF16),
            jax.ShapeDtypeStruct((29, 48), F32),
            jax.ShapeDtypeStruct((3, 192), F32),
        ],
        scratch_shapes=[pltpu.VMEM((4, GROUPS, PARTS, TILE, CHUNK), BF16), pltpu.SemaphoreType.DMA((4, GROUPS, PARTS)), pltpu.SemaphoreType.DMA((4, GROUPS, PARTS, 5))],
        name="unpack",
    )(full, small_full, nw_s)


def solution(mesh):
    grad_spec = P("data", None, None)
    shard_spec = P(None, "data")
    full_spec = P(None, None)

    def local_step(*banks):
        grads, weights, firsts, seconds = (banks[n:n + 4] for n in range(0, len(banks), 4))
        by_wide, by_vec = (x[0].reshape(x.shape[1], DEVICES, -1) for x in grads[2:])
        by_wide = by_wide.reshape(GROUPS, DEVICES, GROUPS, HALF).transpose(1, 2, 0, 3)
        by_wide = jnp.pad(by_wide, ((0, 0), (0, 1), (0, TILE - GROUPS), (0, 0))).reshape(DEVICES, SMALL[0], HALF)
        by_vec = jnp.pad(by_vec.transpose(1, 0, 2), ((0, 0), (0, GROUPS), (0, HALF - by_vec.shape[2])))
        g_small = jnp.concatenate([by_vec, by_wide], axis=2)
        gs_a, gs_m, gs_s, clip = reduce_call(grads[0], grads[1], g_small)
        attn, mlp, wide, vec = zip(weights, firsts, seconds)
        outs = update_call((gs_a,) + attn, (gs_m,) + mlp, clip, gs_s, *vec, *wide)
        nm_a, nv_a, nm_m, nv_m, nm_vec, nv_vec, nm_wide, nv_wide = outs[:8]
        full, small_full, nw_a, nw_m, nw_s = gather_call(weights[0], nm_a, nv_a, weights[1], nm_m, nv_m, *outs[8:])
        rep_a, rep_m, rep_vec, rep_wide, nw_vec, nw_wide = unpack_call(full, small_full, nw_s)
        return (rep_a, rep_m, rep_wide, rep_vec, nw_a, nw_m, nw_wide, nw_vec,
                nm_a, nm_m, nm_wide, nm_vec, nv_a, nv_m, nv_wide, nv_vec)

    return jax.shard_map(local_step, mesh=mesh, in_specs=(grad_spec,) * 4 + (shard_spec,) * 12, out_specs=(full_spec,) * 4 + (shard_spec,) * 12, check_vma=False)
```

```python
import functools

import jax
import jax.numpy as jnp
from jax import lax
from jax.experimental import pallas as pl
from jax.experimental.pallas import tpu as pltpu
from jax.sharding import PartitionSpec as P

STEP_NUMBER = 10
LEARN_RATE = 0.04
BETA_FIRST = 0.9
BETA_SECOND = 0.999
EPSILON = 1e-6
WEIGHT_DECAY = 0.01
MAX_NORM = 1.0
FIRST_SCALE = 1.0 / (1.0 - BETA_FIRST ** STEP_NUMBER)
SECOND_SCALE = 1.0 / (1.0 - BETA_SECOND ** STEP_NUMBER)

MESH = pl.DeviceIdType.MESH
F32 = jnp.float32
BF16 = jnp.bfloat16
DEVICES = 16
LANES = 128
KT = 48
CHUNK = 3 * KT * LANES
ATTN_COLS = 2 * KT * LANES
MLP_COLS = 4 * KT * LANES
ATTN_W = 3 * ATTN_COLS
MLP_W = 6 * MLP_COLS
STEP = 4 * LANES
STEPS = KT * LANES // STEP
TILE = 8
A_ROWS = 12
M_ROWS = 6
GROUPS = 3
QUADS = 4
PARTS = 3
HALF = LANES // 2
VMEM_LIMIT = 67043328
LAST = 3
ANTIPODE = 7
FIRST_OWNERS = 10
SMALL = (32, 128)
WEIGHT = (1, 2, 4)
BLOCKS = [slice(row, row + TILE) for row in range(0, SMALL[0], TILE)]
ORDER = [(g, j) for j in range(GROUPS) for g in range(GROUPS)]
AXES = ((0, 1, 2), (1, 2, 0), (2, 0, 1))


def position():
    me = lax.axis_index("data")
    bits = [lax.rem(me // 2, 2), lax.rem(me // 4, 2), lax.rem(me // 8, 2)]
    return me, lax.rem(me, 2), bits


def flip(bit, by):
    return bit + by - 2 * bit * by


def chip_at(bits, flips):
    total = 0
    for axis in range(GROUPS):
        total = total + flip(bits[axis], flips[axis]) * WEIGHT[axis]
    return total


def flips_of(group, first, second, third):
    flips = [0, 0, 0]
    for axis, by in zip(AXES[group], (first, second, third)):
        flips[axis] = by
    return flips


def columns(group, part, owner):
    if part == 0:
        start = owner * ATTN_W + group * ATTN_COLS
        return pl.ds(pl.multiple_of(start, ATTN_COLS), ATTN_COLS)
    start = owner * MLP_W + group * 2 * MLP_COLS + (part - 1) * MLP_COLS
    return pl.ds(pl.multiple_of(start, MLP_COLS), MLP_COLS)


def signal_all(me):
    barrier = pltpu.get_barrier_semaphore()

    @pl.loop(1, DEVICES)
    def _(t):
        pl.semaphore_signal(barrier, inc=1, device_id=(lax.rem(me + t, DEVICES),), device_id_type=MESH)

    pl.semaphore_wait(barrier, DEVICES - 1)


def spread(me, source, slots, send_sem, recv_sem):
    def copy(t):
        peer = lax.rem(me + t, DEVICES)
        return pltpu.make_async_remote_copy(
            src_ref=source(peer), dst_ref=slots.at[me], send_sem=send_sem.at[t], recv_sem=recv_sem.at[me],
            device_id=(peer,), device_id_type=MESH)

    @pl.loop(1, DEVICES)
    def _(t):
        copy(t).start()


def gather_wait(me, source, slots, send_sem, recv_sem):
    @pl.loop(1, DEVICES)
    def _(t):
        peer = lax.rem(me + t, DEVICES)
        pltpu.make_async_remote_copy(
            src_ref=source(peer), dst_ref=slots.at[peer], send_sem=send_sem.at[t], recv_sem=recv_sem.at[peer],
            device_id=(peer,), device_id_type=MESH).wait()


def put_cols(ref, lo, step, value):
    ref[:, pl.ds(pl.multiple_of(lo * LANES + step * STEP, STEP), STEP)] = value


def pack_rows(part, load, put):
    if part == 0:
        a, b = load(0), load(KT)
        put(0, a[:TILE])
        put(KT, b[:TILE])
        put(2 * KT, jnp.concatenate([a[TILE:], b[TILE:]], axis=0))
    else:
        d = load(3 * KT)
        for t in range(GROUPS):
            put(t * KT, jnp.concatenate([load(t * KT), d[2 * t:2 * t + 2]], axis=0))


def pack_sum(part, own, partner, out, extra):
    @pl.loop(0, STEPS)
    def _(step):
        def cols(lo):
            return pl.ds(pl.multiple_of(lo * LANES + step * STEP, STEP), STEP)

        def put(lo, value):
            if extra is not None:
                value = value + extra[:, cols(lo)]
            put_cols(out, lo, step, value)

        pack_rows(part, lambda lo: own[:, cols(lo)].astype(F32) + partner[:, cols(lo)].astype(F32), put)


def fold(x):
    return sum(x[:, l:l + LANES] for l in range(0, x.shape[1], LANES))


def reduce_kernel(ga, gm, gsmall, pa, pm, gs_a, gs_m, small_out, clip_out,
                  sbuf, r1, r2, r3, raw_a, raw_m, small_slots, norm_slots, acc,
                  d_send, d_recv, s1, q1, s2, q2, s3, q3, load_sem, out_sem, t_send, t_recv, n_send, n_recv):
    me, core, bits = position()
    partner = me + 1 - 2 * core
    signal_all(me)

    def neighbour(axis):
        return me + (2, 4, 8)[axis] * (1 - 2 * bits[axis])


    def owner_chip(half, i, g):
        return chip_at(bits, flips_of(g, 1 - half, 1 - i // 2, 1 - lax.rem(i, 2)))

    def pair_copy(half, i, g, j):
        chip = owner_chip(half, i, g)
        src = (ga, gm)[j > 0].at[0, :, columns(g, j, 2 * chip + 1 - core)]
        dst = (pa, pm)[j > 0].at[:, columns(g, j, chip)]
        return pltpu.make_async_remote_copy(
            src_ref=src, dst_ref=dst, send_sem=d_send.at[half, i, g, j], recv_sem=d_recv.at[half, i, g, j],
            device_id=(partner,), device_id_type=MESH)

    for half in range(2):
        @pl.loop(0, 4)
        def _(i):
            for g, j in ORDER:
                pair_copy(half, i, g, j).start()
        if half == 0:
            spread(me, lambda peer: gsmall.at[peer], small_slots, t_send, t_recv)

    def loads(half, i, g, j, slot):
        chip = owner_chip(half, i, g)
        buf = (raw_a, raw_m)[j > 0]
        own = pltpu.make_async_copy((ga, gm)[j > 0].at[0, :, columns(g, j, 2 * chip + core)], buf.at[slot, 0], load_sem.at[slot, 0])
        par = pltpu.make_async_copy((pa, pm)[j > 0].at[:, columns(g, j, chip)], buf.at[slot, 1], load_sem.at[slot, 1])
        return own, par

    def start_loads(half, i, g, j, slot):
        own, par = loads(half, i, g, j, slot)
        own.start()
        pair_copy(half, i, g, j).wait_recv()
        par.start()

    def send(axis, src, dst, ss, rs):
        return pltpu.make_async_remote_copy(src_ref=src, dst_ref=dst, send_sem=ss, recv_sem=rs,
                                            device_id=(neighbour(axis),), device_id_type=MESH)

    def send1(i, g, j):
        return send(AXES[g][0], sbuf.at[g, i, j], r1.at[g, i, j], s1.at[g, i, j], q1.at[g, i, j])

    def send2(i, g, j):
        return send(AXES[g][1], r1.at[g, i, j], r2.at[g, i, j], s2.at[g, i, j], q2.at[g, i, j])

    def send3(g, j):
        return send(AXES[g][2], r2.at[g, 0, j], r3.at[g, j], s3.at[g, j], q3.at[g, j])

    def sweep(half, i, use):
        start_loads(half, i, *ORDER[0], 0)
        for n, (g, j) in enumerate(ORDER):
            if n + 1 < len(ORDER):
                start_loads(half, i, *ORDER[n + 1], (n + 1) % 2)
            for copy in loads(half, i, g, j, n % 2):
                copy.wait()
            buf = (raw_a, raw_m)[j > 0]
            use(i, g, j, buf.at[n % 2, 0], buf.at[n % 2, 1])

    def first(i, g, j, own, par):
        pack_sum(j, own, par, sbuf.at[g, i, j], None)
        send1(i, g, j).start()

    @pl.loop(0, 4)
    def _(i):
        sweep(0, i, first)

    def second(i, g, j, own, par):
        send1(i, g, j).wait_recv()
        pack_sum(j, own, par, r1.at[g, i, j], r1.at[g, i, j])

    def second_send(i, g, j, own, par):
        second(i, g, j, own, par)
        send2(i, g, j).start()

    @pl.loop(0, 2)
    def _(i):
        sweep(1, i, second_send)

    @pl.loop(2, 4)
    def _(i):
        sweep(1, i, second)

    def add_into(dst, src):
        @pl.loop(0, CHUNK // STEP // 2)
        def _(step):
            cols = pl.ds(pl.multiple_of(step * STEP * 2, STEP * 2), STEP * 2)
            dst[:, cols] = dst[:, cols] + src[:, cols]

    for i in range(2):
        for g, j in ORDER:
            send2(i, g, j).wait_recv()
            add_into(r2.at[g, i, j], r1.at[g, 2 + i, j])
            if i == 0:
                send3(g, j).start()

    gather_wait(me, lambda peer: gsmall.at[peer], small_slots, t_send, t_recv)
    small_slots[me] = gsmall[me]
    small = jnp.zeros(SMALL, F32)
    for slot in range(DEVICES):
        small = small + small_slots[slot].astype(F32)
    small = small * (1.0 / DEVICES)
    small_out[...] = small
    sq = small * small
    acc[...] = sum(sq[rows] for rows in BLOCKS)

    def out_copies(g, j):
        return [pltpu.make_async_copy(r3.at[(g, j) + src], (gs_a, gs_m)[j > 0].at[dst], out_sem.at[g, j, n])
                for n, (src, dst) in enumerate(unpack_moves(g, j, 0))]

    for g, j in ORDER:
        send3(g, j).wait_recv()

        def body(step, sums):
            cols = pl.ds(pl.multiple_of(step * STEP * 2, STEP * 2), STEP * 2)
            value = (r3[g, j, :, cols] + r2[g, 1, j, :, cols]) * (1.0 / DEVICES)
            r3[g, j, :, cols] = value
            return sums + value * value

        sums = lax.fori_loop(0, CHUNK // STEP // 2, body, jnp.zeros((TILE, STEP * 2), F32))
        acc[...] += fold(sums)
        for copy in out_copies(g, j):
            copy.start()

    norm_slots[me] = acc[...]
    spread(me, lambda peer: acc, norm_slots, n_send, n_recv)
    gather_wait(me, lambda peer: acc, norm_slots, n_send, n_recv)
    total = jnp.sum(sum(norm_slots[slot] for slot in range(DEVICES)), axis=(0, 1), keepdims=True)
    clip_out[...] = jnp.broadcast_to(jnp.minimum(1.0, MAX_NORM / jnp.sqrt(total)), (TILE, LANES))

    for g, j in ORDER:
        for copy in out_copies(g, j):
            copy.wait()
        send3(g, j).wait_send()
        for i in range(2):
            send2(i, g, j).wait_send()

    @pl.loop(0, 4)
    def _(i):
        for g, j in ORDER:
            send1(i, g, j).wait_send()
            pair_copy(0, i, g, j).wait_send()
            pair_copy(1, i, g, j).wait_send()


def reduce_call(ga, gm, gsmall):
    hbm = pl.BlockSpec(memory_space=pl.ANY)
    vmem = pl.BlockSpec(memory_space=pltpu.VMEM)
    dma = pltpu.SemaphoreType.DMA
    outs = pl.pallas_call(
        reduce_kernel,
        out_shape=[
            jax.ShapeDtypeStruct((A_ROWS, 8 * ATTN_W), BF16),
            jax.ShapeDtypeStruct((M_ROWS, 8 * MLP_W), BF16),
            jax.ShapeDtypeStruct((A_ROWS, ATTN_W), F32),
            jax.ShapeDtypeStruct((M_ROWS, MLP_W), F32),
            jax.ShapeDtypeStruct(SMALL, F32),
            jax.ShapeDtypeStruct((TILE, LANES), F32),
        ],
        in_specs=[hbm, hbm, vmem],
        out_specs=[hbm] * QUADS + [vmem] * 2,
        scratch_shapes=[
            pltpu.VMEM((GROUPS, QUADS, PARTS, TILE, CHUNK), F32),
            pltpu.VMEM((GROUPS, QUADS, PARTS, TILE, CHUNK), F32),
            pltpu.VMEM((GROUPS, 2, PARTS, TILE, CHUNK), F32),
            pltpu.VMEM((GROUPS, PARTS, TILE, CHUNK), F32),
            pltpu.VMEM((2, 2, A_ROWS, ATTN_COLS), BF16),
            pltpu.VMEM((2, 2, M_ROWS, MLP_COLS), BF16),
            pltpu.VMEM((DEVICES,) + SMALL, BF16),
            pltpu.VMEM((DEVICES, TILE, LANES), F32),
            pltpu.VMEM((TILE, LANES), F32),
            dma((2, QUADS, GROUPS, PARTS)), dma((2, QUADS, GROUPS, PARTS)),
            dma((GROUPS, QUADS, PARTS)), dma((GROUPS, QUADS, PARTS)),
            dma((GROUPS, 2, PARTS)), dma((GROUPS, 2, PARTS)),
            dma((GROUPS, PARTS)), dma((GROUPS, PARTS)),
            dma((2, 2)), dma((GROUPS, PARTS, 5)),
            dma((DEVICES,)), dma((DEVICES,)), dma((DEVICES,)), dma((DEVICES,)),
        ],
        compiler_params=pltpu.CompilerParams(collective_id=0, has_side_effects=True, vmem_limit_bytes=VMEM_LIMIT),
        name="reduce_scatter",
    )(ga, gm, gsmall)
    return outs[2:]


def moments(g, m, v, clip):
    return (BETA_FIRST * m + ((1.0 - BETA_FIRST) * clip) * g,
            BETA_SECOND * v + ((1.0 - BETA_SECOND) * (clip * clip)) * (g * g))


def direction(w, new_m, new_v):
    return (new_m * FIRST_SCALE) / (jnp.sqrt(new_v * SECOND_SCALE) + EPSILON) + WEIGHT_DECAY * w


def chunk_columns(g, j):
    n, width = (g, ATTN_COLS) if j == 0 else (2 * g + j - 1, MLP_COLS)
    return n, pl.ds(n * width, width)


def wide_pieces(ref):
    return [ref[rows.start:rows.start + GROUPS, HALF:] for rows in BLOCKS[:GROUPS]]


def update_kernel(*refs):
    banks, (clip, gs_s), vec, wide = (refs[:4], refs[4:8]), refs[8:10], refs[10:13], refs[13:16]
    outs = refs[16:18], refs[18:20]
    small_outs, u_s, w_s, sums = (refs[20:22], refs[22:24]), refs[24], refs[25], (refs[26:28], refs[28:30])
    bufs, load_sem, out_sem = refs[30:32], refs[32], refs[33]

    def loads(g, j):
        n, cols = chunk_columns(g, j)
        return [pltpu.make_async_copy(ref.at[:, cols], bufs[j > 0].at[n, k], load_sem.at[g, j, k]) for k, ref in enumerate(banks[j > 0])]

    def stores(g, j):
        n, cols = chunk_columns(g, j)
        return [pltpu.make_async_copy(bufs[j > 0].at[n, 2 + k], ref.at[:, cols], out_sem.at[g, j, k]) for k, ref in enumerate(outs[j > 0])]

    for g, j in ORDER:
        for copy in loads(g, j):
            copy.start()

    c = clip[0:1, 0:1]
    u_s[...] = jnp.zeros(SMALL, F32)
    w_s[...] = jnp.zeros(SMALL, F32)
    grads = gs_s[:vec[0].shape[0], :vec[0].shape[1]], jnp.concatenate(wide_pieces(gs_s), axis=1)
    for k, (grad, (w, m, v)) in enumerate(zip(grads, (vec, wide))):
        w = w[...]
        new = moments(grad, m[...], v[...], c)
        for ref, value in zip(small_outs[k], new):
            ref[...] = value
        for ref, value in ((u_s, direction(w, *new)), (w_s, w)):
            if k == 0:
                ref[:value.shape[0], :value.shape[1]] = value
            else:
                for t, rows in enumerate(BLOCKS[:GROUPS]):
                    ref[rows.start:rows.start + GROUPS, HALF:] = value[:, t * HALF:(t + 1) * HALF]

    totals = [[jnp.zeros((rows, LANES), F32)] * 2 for rows in (A_ROWS, M_ROWS)]
    for g, j in ORDER:
        for copy in loads(g, j):
            copy.wait()
        buf, n = bufs[j > 0], chunk_columns(g, j)[0]
        width = STEP * (1 + (j > 0))

        def body(step, total):
            cols = pl.ds(pl.multiple_of(step * width, width), width)
            grad, w, m, v = (buf[n, k, :, cols] for k in range(4))
            new = moments(grad, m, v, c)
            for k in range(2):
                buf[n, 2 + k, :, cols] = new[k]
            return tuple(x + fold(y * y) for x, y in zip(total, (direction(w, *new), w)))

        totals[j > 0] = lax.fori_loop(0, buf.shape[3] // width, body, tuple(totals[j > 0]))
        for copy in stores(g, j):
            copy.start()
    for pair, total in zip(sums, totals):
        for ref, value in zip(pair, total):
            ref[...] = value
    for g, j in ORDER:
        for copy in stores(g, j):
            copy.wait()


def update_call(attn, mlp, *small):
    def whole(shape):
        return pl.BlockSpec(shape, lambda n: (0, 0))

    hbm = pl.BlockSpec(memory_space=pl.ANY)
    outs = [small[2].shape] * 2 + [small[5].shape] * 2 + [SMALL] * 2 + [(A_ROWS, LANES)] * 2 + [(M_ROWS, LANES)] * 2
    return pl.pallas_call(
        update_kernel,
        grid=(1,),
        in_specs=[hbm] * 8 + [whole(x.shape) for x in small],
        out_specs=[hbm] * QUADS + [whole(shape) for shape in outs],
        out_shape=[jax.ShapeDtypeStruct(shape, F32) for shape in [(A_ROWS, ATTN_W)] * 2 + [(M_ROWS, MLP_W)] * 2 + outs],
        scratch_shapes=[
            pltpu.VMEM((GROUPS, QUADS, A_ROWS, ATTN_COLS), F32),
            pltpu.VMEM((2 * GROUPS, QUADS, M_ROWS, MLP_COLS), F32),
            pltpu.SemaphoreType.DMA((GROUPS, PARTS, 4)),
            pltpu.SemaphoreType.DMA((GROUPS, PARTS, 2)),
        ],
        compiler_params=pltpu.CompilerParams(vmem_limit_bytes=VMEM_LIMIT),
        name="update",
    )(*attn, *mlp, *small)


def gather_kernel(*rest):
    banks, rest = (rest[:3], rest[3:6]), rest[6:]
    stats, (full, small_full, nw_a, nw_m, nw_s) = rest[:6], rest[9:14]
    last, stat_bufs, rest = rest[6:9], rest[14:20], rest[20:]
    (sbuf, keep, st_a, st_m, tile, slots, small_buf, x_send, x_recv, d_send, d_recv,
     own_sem, new_sem, keep_in, keep_out, load_sem, stat_sem, n_send, n_recv, t_send, t_recv) = rest
    u_s, w_s, uu_a, ww_a, uu_m, ww_m = stat_bufs
    me, core, bits = position()
    partner = me + 1 - 2 * core
    stat_copies = [pltpu.make_async_copy(src, dst, stat_sem.at[n]) for n, (src, dst) in enumerate(zip(stats, stat_bufs))]
    for copy in stat_copies:
        copy.start()
    signal_all(me)

    def chunk(g, j):
        return (st_a, st_m)[j > 0], *chunk_columns(g, j)

    def loads(g, j):
        buf, n, cols = chunk(g, j)
        return [pltpu.make_async_copy(ref.at[:, cols], buf.at[n, k], load_sem.at[g, j, k]) for k, ref in enumerate(banks[j > 0])]

    for copy in stat_copies:
        copy.wait()
    for g, j in ORDER:
        for copy in loads(g, j):
            copy.start()

    lane = lax.broadcasted_iota(jnp.int32, (TILE, LANES), 1)
    out = jnp.zeros((TILE, LANES), F32)

    def pad8(x):
        return jnp.concatenate([x, jnp.zeros((8 - x.shape[0], x.shape[1]), F32)], axis=0)

    for k, (a, m, s) in enumerate([(uu_a, uu_m, u_s), (ww_a, ww_m, w_s)]):
        a, m, s = a[...], m[...], s[...] * s[...]
        vec = jnp.where(lax.broadcasted_iota(jnp.int32, SMALL, 1) < HALF, s, 0.0)
        wide = s - vec
        blocks = [a[:TILE], pad8(a[TILE:]), pad8(m)] + [vec[rows] for rows in BLOCKS] + [sum(wide[rows] for rows in BLOCKS)]
        for l, block in enumerate(blocks):
            out = jnp.where(lane == TILE * k + l, jnp.sum(block, axis=1, keepdims=True), out)
    tile[...] = out
    slots[me] = out
    spread(me, lambda peer: tile, slots, n_send, n_recv)
    gather_wait(me, lambda peer: tile, slots, n_send, n_recv)
    root = jnp.sqrt(sum(slots[slot] for slot in range(DEVICES)))
    ratio = [LEARN_RATE * (root[:, 8 + l:9 + l] / root[:, l:l + 1]) for l in range(8)]

    def place(g, r, j):
        owner = 2 * chip_at(bits, flips_of(g, lax.rem(r, 2), lax.rem(r // 2, 2), r // 4)) + core
        return full.at[owner, g, j]

    def landing(g, r, j, arrived):
        return last[g].at[j] if arrived is LAST else place(g, r, j)

    def keep_copies(g, j):
        return (pltpu.make_async_copy(last[g].at[j], keep.at[g, j], keep_in.at[g, j]),
                pltpu.make_async_copy(keep.at[g, j], place(g, LAST, j), keep_out.at[g, j]))

    def copy_to(g, r, j, to, arrived, sends, recvs, src, dst=None):
        return pltpu.make_async_remote_copy(
            src_ref=src, dst_ref=place(g, r, j) if dst is None else dst, send_sem=sends.at[g, arrived, j], recv_sem=recvs.at[g, arrived, j],
            device_id=(to,), device_id_type=MESH)

    def forward(g, r, j, step, src=None):
        axis = AXES[g][step]
        to = me + WEIGHT[axis] * 2 * (1 - 2 * bits[axis])
        arrived = r + WEIGHT[step]
        copy_to(g, r, j, to, arrived, x_send, x_recv, place(g, r, j) if src is None else src, landing(g, r, j, arrived)).start()

    def to_partner(g, r, j, src=None):
        return copy_to(g, r, j, partner, r, d_send, d_recv, place(g, r, j) if src is None else src)

    def arrival(g, r, j):
        return copy_to(g, r, j, partner, r, x_send, x_recv, place(g, r, j), landing(g, r, j, r))

    def own_copy(g, j):
        return pltpu.make_async_copy(sbuf.at[g, j], place(g, 0, j), own_sem.at[g, j])

    def new_copy(g, j):
        buf, n, cols = chunk(g, j)
        return pltpu.make_async_copy(buf.at[n, 0], (nw_a, nw_m)[j > 0].at[:, cols], new_sem.at[g, j])

    for g, j in ORDER:
        for copy in loads(g, j):
            copy.wait()
        buf, n, _ = chunk(g, j)
        scale = jnp.concatenate([ratio[0], ratio[1][0:4]], axis=0) if j == 0 else ratio[2][0:6]

        @pl.loop(0, STEPS)
        def _(step):
            def new(lo):
                cols = pl.ds(pl.multiple_of(lo * LANES + step * STEP, STEP), STEP)
                w, m, v = (buf[n, k, :, cols] for k in range(GROUPS))
                value = w - scale * direction(w, m, v)
                buf[n, 0, :, cols] = value
                return value

            pack_rows(j, new, lambda lo, value: put_cols(sbuf.at[g, j], lo, step, value.astype(BF16)))

        forward(g, 0, j, 0, sbuf.at[g, j])
        own_copy(g, j).start()
        new_copy(g, j).start()

    for step in (1, 2):
        for g, j in ORDER:
            forward(g, 0, j, step, sbuf.at[g, j])
    for g, j in ORDER:
        to_partner(g, 0, j, sbuf.at[g, j]).start()
    for rows, scale in zip(BLOCKS, ratio[3:]):
        nw_s[rows] = w_s[rows] - jnp.where(lane < HALF, scale, ratio[7]) * u_s[rows]
    small_buf[...] = nw_s[...].astype(BF16)
    spread(me, lambda peer: small_buf, small_full, t_send, t_recv)

    def receive(r, steps):
        for g, j in ORDER:
            arrival(g, r, j).wait_recv()
            for step in steps:
                forward(g, r, j, step)
            to_partner(g, r, j, landing(g, r, j, r)).start()
            if r is LAST:
                keep_copies(g, j)[0].start()

    receive(1, (1, 2))
    receive(2, (2,))
    receive(LAST, ())

    @pl.loop(LAST + 1, ANTIPODE)
    def _(r):
        receive(r, ())

    for g, j in ORDER:
        into, out_of = keep_copies(g, j)
        into.wait()
        out_of.start()

    gather_wait(me, lambda peer: small_buf, small_full, t_send, t_recv)
    small_full[me] = small_buf[...]
    for g, j in ORDER:
        own_copy(g, j).wait()
        keep_copies(g, j)[1].wait()
        new_copy(g, j).wait()

    @pl.loop(0, ANTIPODE)
    def _(r):
        for g, j in ORDER:
            to_partner(g, r, j).wait()

    @pl.loop(1, ANTIPODE)
    def _(r):
        for g, j in ORDER:
            arrival(g, r, j).wait_send()


def gather_call(*args):
    hbm = pl.BlockSpec(memory_space=pl.ANY)
    vmem = pl.BlockSpec(memory_space=pltpu.VMEM)
    dma = pltpu.SemaphoreType.DMA
    sems = [dma((GROUPS, TILE, PARTS))] * 4 + [dma((GROUPS, PARTS))] * 4 + [dma((GROUPS, PARTS, GROUPS)), dma((6,))] + [dma((DEVICES,))] * 4
    return pl.pallas_call(
        gather_kernel,
        out_shape=[jax.ShapeDtypeStruct((PARTS, TILE, CHUNK), BF16)] * GROUPS + [
            jax.ShapeDtypeStruct((DEVICES, GROUPS, PARTS, TILE, CHUNK), BF16),
            jax.ShapeDtypeStruct((DEVICES,) + SMALL, BF16),
            jax.ShapeDtypeStruct((A_ROWS, ATTN_W), F32),
            jax.ShapeDtypeStruct((M_ROWS, MLP_W), F32),
            jax.ShapeDtypeStruct(SMALL, F32),
        ],
        in_specs=[hbm] * len(args),
        out_specs=[hbm] * (GROUPS + 1) + [vmem, hbm, hbm, vmem],
        scratch_shapes=[pltpu.VMEM(x.shape, F32) for x in args[6:]] + [
            pltpu.VMEM((GROUPS, PARTS, TILE, CHUNK), BF16),
            pltpu.VMEM((GROUPS, PARTS, TILE, CHUNK), BF16),
            pltpu.VMEM((3, 3, A_ROWS, ATTN_COLS), F32),
            pltpu.VMEM((M_ROWS, 3, M_ROWS, MLP_COLS), F32),
            pltpu.VMEM((TILE, LANES), F32),
            pltpu.VMEM((DEVICES, TILE, LANES), F32),
            pltpu.VMEM(SMALL, BF16),
        ] + sems,
        compiler_params=pltpu.CompilerParams(collective_id=1, has_side_effects=True, vmem_limit_bytes=VMEM_LIMIT),
        name="all_gather",
    )(*args)


def unpack_moves(g, j, owner):
    if j == 0:
        start = owner * ATTN_W + g * ATTN_COLS
        moves = [(0, 8, 0, 2, 0, 0)] + [(4 * t, 4, 2, 1, 8, t) for t in range(2)]
    else:
        start = owner * MLP_W + (2 * g + j - 1) * MLP_COLS
        moves = [(0, 4, 0, 3, 0, 0), (4, 2, 0, 3, 4, 0)] + [(M_ROWS, 2, t, 1, 2 * t, 3) for t in range(GROUPS)]
    third = KT * LANES
    for row, rows, lo, width, to, at in moves:
        cols = pl.ds(pl.multiple_of(start + at * third, third), width * third)
        yield (pl.ds(row, rows), pl.ds(lo * third, width * third)), (pl.ds(to, rows), cols)


def stream(count, owner_of, source, reps, buf, load_sem, out_sem):
    def loads(t):
        slot = lax.rem(t, buf.shape[0])
        return [pltpu.make_async_copy(source(t, g, j), buf.at[slot, g, j], load_sem.at[slot, g, j]) for g, j in ORDER]

    def outs(t, g, j):
        slot = lax.rem(t, buf.shape[0])
        return [pltpu.make_async_copy(buf.at[(slot, g, j) + src], reps[j > 0].at[dst], out_sem.at[slot, g, j, n])
                for n, (src, dst) in enumerate(unpack_moves(g, j, owner_of(t)))]

    def begin(t):
        for copy in loads(t):
            copy.start()

    def move(t):
        for (g, j), copy in zip(ORDER, loads(t)):
            copy.wait()
            for out in outs(t, g, j):
                out.start()

    def drain(t):
        for g, j in ORDER:
            for out in outs(t, g, j):
                out.wait()

    begin(0)
    begin(1)
    if count > 2:
        @pl.loop(0, count)
        def _(t):
            pl.when(t >= 2)(lambda: drain(t - 2))
            pl.when(t < count - 2)(lambda: begin(t + 2))
            move(t)
    else:
        move(0)
        move(1)
    drain(count - 2)
    drain(count - 1)


def far_owner(skip):
    _, core, bits = position()
    far = 2 * chip_at(bits, (1, 1, 1))
    return lambda t: lax.rem(far + skip + t, DEVICES), far, core


def unpack_kernel(full, small_full, nw_s, rep_a, rep_m, rep_vec, rep_wide, nw_vec, nw_wide, *scratch):
    owner_of = far_owner(2)[0]
    stream(FIRST_OWNERS, owner_of, lambda t, g, j: full.at[owner_of(t), g, j], (rep_a, rep_m), *scratch)
    vec = nw_vec.shape
    nw_vec[...] = nw_s[:vec[0], :vec[1]]
    nw_wide[...] = jnp.concatenate(wide_pieces(nw_s), axis=1)
    shares = [small_full[n].astype(F32) for n in range(DEVICES)]
    rep_vec[...] = jnp.concatenate([x[:vec[0], :vec[1]] for x in shares], axis=1).astype(BF16)
    rep_wide[...] = jnp.concatenate([piece for x in shares for piece in wide_pieces(x)], axis=1).astype(BF16)


def more_kernel(full, *refs):
    owner_of = far_owner(2 + FIRST_OWNERS)[0]
    stream(DEVICES - 2 - FIRST_OWNERS, owner_of, lambda t, g, j: full.at[owner_of(t), g, j], refs[-5:-3], *refs[-3:])


def far_kernel(*refs):
    _, far, core = far_owner(0)
    stream(2, lambda t: far + flip(core, t), lambda t, g, j: refs[t * GROUPS + g].at[j], refs[-5:-3], *refs[-3:])


REPLICAS = [jax.ShapeDtypeStruct((A_ROWS, DEVICES * ATTN_W), BF16), jax.ShapeDtypeStruct((M_ROWS, DEVICES * MLP_W), BF16)]


def stream_call(kernel, name, ins, vmem_ins=(), vmem_outs=(), reps=()):
    hbm = pl.BlockSpec(memory_space=pl.ANY)
    vmem = pl.BlockSpec(memory_space=pltpu.VMEM)
    dma = pltpu.SemaphoreType.DMA
    count = len(ins) + len(vmem_ins)
    return pl.pallas_call(
        kernel,
        in_specs=[hbm] * len(ins) + [vmem] * len(vmem_ins) + [hbm] * len(reps),
        out_specs=[hbm] * 2 + [vmem] * len(vmem_outs),
        out_shape=REPLICAS + list(vmem_outs),
        scratch_shapes=[pltpu.VMEM((QUADS, GROUPS, PARTS, TILE, CHUNK), BF16), dma((QUADS, GROUPS, PARTS)), dma((QUADS, GROUPS, PARTS, 5))],
        input_output_aliases={count + n: n for n in range(len(reps))},
        cost_estimate=pl.CostEstimate(flops=10 ** 9, bytes_accessed=2 ** 26, transcendentals=0),
        compiler_params=pltpu.CompilerParams(vmem_limit_bytes=VMEM_LIMIT),
        name=name,
    )(*ins, *vmem_ins, *reps)


def swap(x, weight):
    return lax.ppermute(x, "data", [(d, d ^ weight) for d in range(DEVICES)])


def solution(mesh):
    grad_spec = P("data", None, None)
    shard_spec = P(None, "data")
    full_spec = P(None, None)

    def local_step(*banks):
        grads, weights, firsts, seconds = (banks[n:n + 4] for n in range(0, len(banks), 4))
        by_wide, by_vec = (x[0].reshape(x.shape[1], DEVICES, -1) for x in grads[2:])
        by_wide = by_wide.reshape(GROUPS, DEVICES, GROUPS, HALF).transpose(1, 2, 0, 3)
        by_wide = jnp.pad(by_wide, ((0, 0), (0, 1), (0, TILE - GROUPS), (0, 0))).reshape(DEVICES, SMALL[0], HALF)
        by_vec = jnp.pad(by_vec.transpose(1, 0, 2), ((0, 0), (0, GROUPS), (0, HALF - by_vec.shape[2])))
        g_small = jnp.concatenate([by_vec, by_wide], axis=2)
        gs_a, gs_m, gs_s, clip = reduce_call(grads[0], grads[1], g_small)
        attn, mlp, wide, vec = zip(weights, firsts, seconds)
        outs = update_call((gs_a,) + attn, (gs_m,) + mlp, clip, gs_s, *vec, *wide)
        nm_a, nv_a, nm_m, nv_m, nm_vec, nv_vec, nm_wide, nv_wide = outs[:8]
        outs = gather_call(weights[0], nm_a, nv_a, weights[1], nm_m, nv_m, *outs[8:])
        last, (full, small_full, nw_a, nw_m, nw_s) = outs[:GROUPS], outs[GROUPS:]
        far = [swap(x, 2 * WEIGHT[axes[2]]) for x, axes in zip(last, AXES)]
        tail = [jax.ShapeDtypeStruct(shape, dtype) for dtype, bank in ((BF16, grads), (F32, weights)) for shape in (bank[3].shape[-2:], bank[2].shape[-2:])]
        rep_a, rep_m, rep_vec, rep_wide, nw_vec, nw_wide = stream_call(unpack_kernel, "unpack", [full], (small_full, nw_s), tail)
        far, rep_a, rep_m = lax.optimization_barrier((far, rep_a, rep_m))
        across = [swap(x, 1) for x in far]
        reps = stream_call(more_kernel, "unpack_more", [full] + far, reps=(rep_a, rep_m))
        rep_a, rep_m = stream_call(far_kernel, "unpack_far", far + across, reps=reps)
        return (rep_a, rep_m, rep_wide, rep_vec, nw_a, nw_m, nw_wide, nw_vec,
                nm_a, nm_m, nm_wide, nm_vec, nv_a, nv_m, nv_wide, nv_vec)

    return jax.shard_map(local_step, mesh=mesh, in_specs=(grad_spec,) * 4 + (shard_spec,) * 12, out_specs=(full_spec,) * 4 + (shard_spec,) * 12, check_vma=False)
```

```python
import functools

import jax
import jax.numpy as jnp
from jax import lax
from jax.experimental import pallas as pl
from jax.experimental.pallas import tpu as pltpu
from jax.sharding import PartitionSpec as P

STEP_NUMBER = 10
LEARN_RATE = 0.04
BETA_FIRST = 0.9
BETA_SECOND = 0.999
EPSILON = 1e-6
WEIGHT_DECAY = 0.01
MAX_NORM = 1.0
FIRST_SCALE = 1.0 / (1.0 - BETA_FIRST ** STEP_NUMBER)
SECOND_SCALE = 1.0 / (1.0 - BETA_SECOND ** STEP_NUMBER)

MESH = pl.DeviceIdType.MESH
F32 = jnp.float32
BF16 = jnp.bfloat16
DEVICES = 16
LANES = 128
KT = 48
CHUNK = 3 * KT * LANES
ATTN_COLS = 2 * KT * LANES
MLP_COLS = 4 * KT * LANES
ATTN_W = 3 * ATTN_COLS
MLP_W = 6 * MLP_COLS
STEP = 4 * LANES
STEPS = KT * LANES // STEP
TILE = 8
A_ROWS = 12
M_ROWS = 6
GROUPS = 3
QUADS = 4
PARTS = 3
HALF = LANES // 2
VMEM_LIMIT = 67043328
LAST = 3
ANTIPODE = 7
FIRST_OWNERS = 10
SMALL = (32, 128)
WEIGHT = (1, 2, 4)
BLOCKS = [slice(row, row + TILE) for row in range(0, SMALL[0], TILE)]
ORDER = [(g, j) for j in range(GROUPS) for g in range(GROUPS)]
AXES = ((0, 1, 2), (1, 2, 0), (2, 0, 1))


def position():
    me = lax.axis_index("data")
    bits = [lax.rem(me // 2, 2), lax.rem(me // 4, 2), lax.rem(me // 8, 2)]
    return me, lax.rem(me, 2), bits


def flip(bit, by):
    return bit + by - 2 * bit * by


def chip_at(bits, flips):
    total = 0
    for axis in range(GROUPS):
        total = total + flip(bits[axis], flips[axis]) * WEIGHT[axis]
    return total


def flips_of(group, first, second, third):
    flips = [0, 0, 0]
    for axis, by in zip(AXES[group], (first, second, third)):
        flips[axis] = by
    return flips


def columns(group, part, owner):
    if part == 0:
        start = owner * ATTN_W + group * ATTN_COLS
        return pl.ds(pl.multiple_of(start, ATTN_COLS), ATTN_COLS)
    start = owner * MLP_W + group * 2 * MLP_COLS + (part - 1) * MLP_COLS
    return pl.ds(pl.multiple_of(start, MLP_COLS), MLP_COLS)


def signal_all(me):
    barrier = pltpu.get_barrier_semaphore()

    @pl.loop(1, DEVICES)
    def _(t):
        pl.semaphore_signal(barrier, inc=1, device_id=(lax.rem(me + t, DEVICES),), device_id_type=MESH)

    pl.semaphore_wait(barrier, DEVICES - 1)


def spread(me, source, slots, send_sem, recv_sem):
    def copy(t):
        peer = lax.rem(me + t, DEVICES)
        return pltpu.make_async_remote_copy(
            src_ref=source(peer), dst_ref=slots.at[me], send_sem=send_sem.at[t], recv_sem=recv_sem.at[me],
            device_id=(peer,), device_id_type=MESH)

    @pl.loop(1, DEVICES)
    def _(t):
        copy(t).start()


def gather_wait(me, source, slots, send_sem, recv_sem):
    @pl.loop(1, DEVICES)
    def _(t):
        peer = lax.rem(me + t, DEVICES)
        pltpu.make_async_remote_copy(
            src_ref=source(peer), dst_ref=slots.at[peer], send_sem=send_sem.at[t], recv_sem=recv_sem.at[peer],
            device_id=(peer,), device_id_type=MESH).wait()


def put_cols(ref, lo, step, value):
    ref[:, pl.ds(pl.multiple_of(lo * LANES + step * STEP, STEP), STEP)] = value


def pack_rows(part, load, put):
    if part == 0:
        a, b = load(0), load(KT)
        put(0, a[:TILE])
        put(KT, b[:TILE])
        put(2 * KT, jnp.concatenate([a[TILE:], b[TILE:]], axis=0))
    else:
        d = load(3 * KT)
        for t in range(GROUPS):
            put(t * KT, jnp.concatenate([load(t * KT), d[2 * t:2 * t + 2]], axis=0))


def pack_sum(part, own, partner, out, extra):
    @pl.loop(0, STEPS)
    def _(step):
        def cols(lo):
            return pl.ds(pl.multiple_of(lo * LANES + step * STEP, STEP), STEP)

        def put(lo, value):
            if extra is not None:
                value = value + extra[:, cols(lo)]
            put_cols(out, lo, step, value)

        pack_rows(part, lambda lo: own[:, cols(lo)].astype(F32) + partner[:, cols(lo)].astype(F32), put)


def fold(x):
    return sum(x[:, l:l + LANES] for l in range(0, x.shape[1], LANES))


def reduce_kernel(ga, gm, gvec, gwide, pa, pm, gs_a, gs_m, small_out, clip_out,
                  sbuf, r1, r2, r3, raw_a, raw_m, raw_vec, raw_wide, block, gsmall, small_slots, norm_slots, acc,
                  d_send, d_recv, s1, q1, s2, q2, s3, q3, load_sem, out_sem, t_send, t_recv, n_send, n_recv, v_sem):
    me, core, bits = position()
    partner = me + 1 - 2 * core
    small_loads = [pltpu.make_async_copy(src.at[0], dst, v_sem.at[n]) for n, (src, dst) in enumerate(((gvec, raw_vec), (gwide, raw_wide)))]
    for copy in small_loads:
        copy.start()
    signal_all(me)

    def neighbour(axis):
        return me + (2, 4, 8)[axis] * (1 - 2 * bits[axis])


    def owner_chip(half, i, g):
        return chip_at(bits, flips_of(g, 1 - half, 1 - i // 2, 1 - lax.rem(i, 2)))

    def pair_copy(half, i, g, j):
        chip = owner_chip(half, i, g)
        src = (ga, gm)[j > 0].at[0, :, columns(g, j, 2 * chip + 1 - core)]
        dst = (pa, pm)[j > 0].at[:, columns(g, j, chip)]
        return pltpu.make_async_remote_copy(
            src_ref=src, dst_ref=dst, send_sem=d_send.at[half, i, g, j], recv_sem=d_recv.at[half, i, g, j],
            device_id=(partner,), device_id_type=MESH)

    for half in range(2):
        @pl.loop(0, 4)
        def _(i):
            for g, j in ORDER:
                pair_copy(half, i, g, j).start()

    def loads(half, i, g, j, slot):
        chip = owner_chip(half, i, g)
        buf = (raw_a, raw_m)[j > 0]
        own = pltpu.make_async_copy((ga, gm)[j > 0].at[0, :, columns(g, j, 2 * chip + core)], buf.at[slot, 0], load_sem.at[slot, 0])
        par = pltpu.make_async_copy((pa, pm)[j > 0].at[:, columns(g, j, chip)], buf.at[slot, 1], load_sem.at[slot, 1])
        return own, par

    def start_loads(half, i, g, j, slot):
        own, par = loads(half, i, g, j, slot)
        own.start()
        pair_copy(half, i, g, j).wait_recv()
        par.start()

    def send(axis, src, dst, ss, rs):
        return pltpu.make_async_remote_copy(src_ref=src, dst_ref=dst, send_sem=ss, recv_sem=rs,
                                            device_id=(neighbour(axis),), device_id_type=MESH)

    def send1(i, g, j):
        return send(AXES[g][0], sbuf.at[g, i, j], r1.at[g, i, j], s1.at[g, i, j], q1.at[g, i, j])

    def send2(i, g, j):
        return send(AXES[g][1], r1.at[g, i, j], r2.at[g, i, j], s2.at[g, i, j], q2.at[g, i, j])

    def send3(g, j):
        return send(AXES[g][2], r2.at[g, 0, j], r3.at[g, j], s3.at[g, j], q3.at[g, j])

    def sweep(half, i, use):
        start_loads(half, i, *ORDER[0], 0)
        for n, (g, j) in enumerate(ORDER):
            if n + 1 < len(ORDER):
                start_loads(half, i, *ORDER[n + 1], (n + 1) % 2)
            for copy in loads(half, i, g, j, n % 2):
                copy.wait()
            buf = (raw_a, raw_m)[j > 0]
            use(i, g, j, buf.at[n % 2, 0], buf.at[n % 2, 1])

    def first(i, g, j, own, par):
        pack_sum(j, own, par, sbuf.at[g, i, j], None)
        send1(i, g, j).start()

    @pl.loop(0, 4)
    def _(i):
        sweep(0, i, first)

    for copy in small_loads:
        copy.wait()
    vec, wide = raw_vec[...].astype(F32), raw_wide[...].astype(F32)
    share = vec.shape[1] // DEVICES
    block[...] = jnp.zeros(SMALL, F32)
    for owner in range(DEVICES):
        block[:vec.shape[0], :share] = vec[:, owner * share:(owner + 1) * share]
        for t, rows in enumerate(BLOCKS[:GROUPS]):
            lane = (owner * GROUPS + t) * HALF
            block[rows.start:rows.start + GROUPS, HALF:] = wide[:, lane:lane + HALF]
        gsmall[owner] = block[...].astype(BF16)
    spread(me, lambda peer: gsmall.at[peer], small_slots, t_send, t_recv)

    def second(i, g, j, own, par):
        send1(i, g, j).wait_recv()
        pack_sum(j, own, par, r1.at[g, i, j], r1.at[g, i, j])

    def second_send(i, g, j, own, par):
        second(i, g, j, own, par)
        send2(i, g, j).start()

    @pl.loop(0, 2)
    def _(i):
        sweep(1, i, second_send)

    @pl.loop(2, 4)
    def _(i):
        sweep(1, i, second)

    def add_into(dst, src):
        @pl.loop(0, CHUNK // STEP // 2)
        def _(step):
            cols = pl.ds(pl.multiple_of(step * STEP * 2, STEP * 2), STEP * 2)
            dst[:, cols] = dst[:, cols] + src[:, cols]

    for i in range(2):
        for g, j in ORDER:
            send2(i, g, j).wait_recv()
            add_into(r2.at[g, i, j], r1.at[g, 2 + i, j])
            if i == 0:
                send3(g, j).start()

    gather_wait(me, lambda peer: gsmall.at[peer], small_slots, t_send, t_recv)
    small_slots[me] = gsmall[me]
    small = jnp.zeros(SMALL, F32)
    for slot in range(DEVICES):
        small = small + small_slots[slot].astype(F32)
    small = small * (1.0 / DEVICES)
    small_out[...] = small
    sq = small * small
    acc[...] = sum(sq[rows] for rows in BLOCKS)

    def out_copies(g, j):
        return [pltpu.make_async_copy(r3.at[(g, j) + src], (gs_a, gs_m)[j > 0].at[dst], out_sem.at[g, j, n])
                for n, (src, dst) in enumerate(unpack_moves(g, j, 0))]

    for g, j in ORDER:
        send3(g, j).wait_recv()

        def body(step, sums):
            cols = pl.ds(pl.multiple_of(step * STEP * 2, STEP * 2), STEP * 2)
            value = (r3[g, j, :, cols] + r2[g, 1, j, :, cols]) * (1.0 / DEVICES)
            r3[g, j, :, cols] = value
            return sums + value * value

        sums = lax.fori_loop(0, CHUNK // STEP // 2, body, jnp.zeros((TILE, STEP * 2), F32))
        acc[...] += fold(sums)
        for copy in out_copies(g, j):
            copy.start()

    norm_slots[me] = acc[...]
    spread(me, lambda peer: acc, norm_slots, n_send, n_recv)
    gather_wait(me, lambda peer: acc, norm_slots, n_send, n_recv)
    total = jnp.sum(sum(norm_slots[slot] for slot in range(DEVICES)), axis=(0, 1), keepdims=True)
    clip_out[...] = jnp.broadcast_to(jnp.minimum(1.0, MAX_NORM / jnp.sqrt(total)), (TILE, LANES))

    for g, j in ORDER:
        for copy in out_copies(g, j):
            copy.wait()
        send3(g, j).wait_send()
        for i in range(2):
            send2(i, g, j).wait_send()

    @pl.loop(0, 4)
    def _(i):
        for g, j in ORDER:
            send1(i, g, j).wait_send()
            pair_copy(0, i, g, j).wait_send()
            pair_copy(1, i, g, j).wait_send()


def reduce_call(*grads):
    hbm = pl.BlockSpec(memory_space=pl.ANY)
    vmem = pl.BlockSpec(memory_space=pltpu.VMEM)
    dma = pltpu.SemaphoreType.DMA
    outs = pl.pallas_call(
        reduce_kernel,
        out_shape=[
            jax.ShapeDtypeStruct((A_ROWS, 8 * ATTN_W), BF16),
            jax.ShapeDtypeStruct((M_ROWS, 8 * MLP_W), BF16),
            jax.ShapeDtypeStruct((A_ROWS, ATTN_W), F32),
            jax.ShapeDtypeStruct((M_ROWS, MLP_W), F32),
            jax.ShapeDtypeStruct(SMALL, F32),
            jax.ShapeDtypeStruct((TILE, LANES), F32),
        ],
        in_specs=[hbm] * QUADS,
        out_specs=[hbm] * QUADS + [vmem] * 2,
        scratch_shapes=[
            pltpu.VMEM((GROUPS, QUADS, PARTS, TILE, CHUNK), F32),
            pltpu.VMEM((GROUPS, QUADS, PARTS, TILE, CHUNK), F32),
            pltpu.VMEM((GROUPS, 2, PARTS, TILE, CHUNK), F32),
            pltpu.VMEM((GROUPS, PARTS, TILE, CHUNK), F32),
            pltpu.VMEM((2, 2, A_ROWS, ATTN_COLS), BF16),
            pltpu.VMEM((2, 2, M_ROWS, MLP_COLS), BF16),
            pltpu.VMEM(grads[2].shape[1:], BF16),
            pltpu.VMEM(grads[3].shape[1:], BF16),
            pltpu.VMEM(SMALL, F32),
            pltpu.VMEM((DEVICES,) + SMALL, BF16),
            pltpu.VMEM((DEVICES,) + SMALL, BF16),
            pltpu.VMEM((DEVICES, TILE, LANES), F32),
            pltpu.VMEM((TILE, LANES), F32),
            dma((2, QUADS, GROUPS, PARTS)), dma((2, QUADS, GROUPS, PARTS)),
            dma((GROUPS, QUADS, PARTS)), dma((GROUPS, QUADS, PARTS)),
            dma((GROUPS, 2, PARTS)), dma((GROUPS, 2, PARTS)),
            dma((GROUPS, PARTS)), dma((GROUPS, PARTS)),
            dma((2, 2)), dma((GROUPS, PARTS, 5)),
            dma((DEVICES,)), dma((DEVICES,)), dma((DEVICES,)), dma((DEVICES,)), dma((2,)),
        ],
        compiler_params=pltpu.CompilerParams(collective_id=0, has_side_effects=True, vmem_limit_bytes=VMEM_LIMIT),
        name="reduce_scatter",
    )(*grads)
    return outs[2:]


def moments(g, m, v, clip):
    return (BETA_FIRST * m + ((1.0 - BETA_FIRST) * clip) * g,
            BETA_SECOND * v + ((1.0 - BETA_SECOND) * (clip * clip)) * (g * g))


def direction(w, new_m, new_v):
    return (new_m * FIRST_SCALE) / (jnp.sqrt(new_v * SECOND_SCALE) + EPSILON) + WEIGHT_DECAY * w


def chunk_columns(g, j):
    n, width = (g, ATTN_COLS) if j == 0 else (2 * g + j - 1, MLP_COLS)
    return n, pl.ds(n * width, width)


def wide_pieces(ref):
    return [ref[rows.start:rows.start + GROUPS, HALF:] for rows in BLOCKS[:GROUPS]]


def update_kernel(*refs):
    banks, (clip, gs_s), vec, wide = (refs[:4], refs[4:8]), refs[8:10], refs[10:13], refs[13:16]
    outs = refs[16:18], refs[18:20]
    small_outs, u_s, w_s, sums = (refs[20:22], refs[22:24]), refs[24], refs[25], (refs[26:28], refs[28:30])
    bufs, load_sem, out_sem = refs[30:32], refs[32], refs[33]

    def loads(g, j):
        n, cols = chunk_columns(g, j)
        return [pltpu.make_async_copy(ref.at[:, cols], bufs[j > 0].at[n, k], load_sem.at[g, j, k]) for k, ref in enumerate(banks[j > 0])]

    def stores(g, j):
        n, cols = chunk_columns(g, j)
        return [pltpu.make_async_copy(bufs[j > 0].at[n, 2 + k], ref.at[:, cols], out_sem.at[g, j, k]) for k, ref in enumerate(outs[j > 0])]

    for g, j in ORDER:
        for copy in loads(g, j):
            copy.start()

    c = clip[0:1, 0:1]
    u_s[...] = jnp.zeros(SMALL, F32)
    w_s[...] = jnp.zeros(SMALL, F32)
    grads = gs_s[:vec[0].shape[0], :vec[0].shape[1]], jnp.concatenate(wide_pieces(gs_s), axis=1)
    for k, (grad, (w, m, v)) in enumerate(zip(grads, (vec, wide))):
        w = w[...]
        new = moments(grad, m[...], v[...], c)
        for ref, value in zip(small_outs[k], new):
            ref[...] = value
        for ref, value in ((u_s, direction(w, *new)), (w_s, w)):
            if k == 0:
                ref[:value.shape[0], :value.shape[1]] = value
            else:
                for t, rows in enumerate(BLOCKS[:GROUPS]):
                    ref[rows.start:rows.start + GROUPS, HALF:] = value[:, t * HALF:(t + 1) * HALF]

    totals = [[jnp.zeros((rows, LANES), F32)] * 2 for rows in (A_ROWS, M_ROWS)]
    for g, j in ORDER:
        for copy in loads(g, j):
            copy.wait()
        buf, n = bufs[j > 0], chunk_columns(g, j)[0]
        width = STEP * (1 + (j > 0))

        def body(step, total):
            cols = pl.ds(pl.multiple_of(step * width, width), width)
            grad, w, m, v = (buf[n, k, :, cols] for k in range(4))
            new = moments(grad, m, v, c)
            for k in range(2):
                buf[n, 2 + k, :, cols] = new[k]
            return tuple(x + fold(y * y) for x, y in zip(total, (direction(w, *new), w)))

        totals[j > 0] = lax.fori_loop(0, buf.shape[3] // width, body, tuple(totals[j > 0]))
        for copy in stores(g, j):
            copy.start()
    for pair, total in zip(sums, totals):
        for ref, value in zip(pair, total):
            ref[...] = value
    for g, j in ORDER:
        for copy in stores(g, j):
            copy.wait()


def update_call(attn, mlp, *small):
    def whole(shape):
        return pl.BlockSpec(shape, lambda n: (0, 0))

    hbm = pl.BlockSpec(memory_space=pl.ANY)
    outs = [small[2].shape] * 2 + [small[5].shape] * 2 + [SMALL] * 2 + [(A_ROWS, LANES)] * 2 + [(M_ROWS, LANES)] * 2
    return pl.pallas_call(
        update_kernel,
        grid=(1,),
        in_specs=[hbm] * 8 + [whole(x.shape) for x in small],
        out_specs=[hbm] * QUADS + [whole(shape) for shape in outs],
        out_shape=[jax.ShapeDtypeStruct(shape, F32) for shape in [(A_ROWS, ATTN_W)] * 2 + [(M_ROWS, MLP_W)] * 2 + outs],
        scratch_shapes=[
            pltpu.VMEM((GROUPS, QUADS, A_ROWS, ATTN_COLS), F32),
            pltpu.VMEM((2 * GROUPS, QUADS, M_ROWS, MLP_COLS), F32),
            pltpu.SemaphoreType.DMA((GROUPS, PARTS, 4)),
            pltpu.SemaphoreType.DMA((GROUPS, PARTS, 2)),
        ],
        compiler_params=pltpu.CompilerParams(vmem_limit_bytes=VMEM_LIMIT),
        name="update",
    )(*attn, *mlp, *small)


def gather_kernel(*rest):
    banks, rest = (rest[:3], rest[3:6]), rest[6:]
    stats, (full, small_full, nw_a, nw_m, nw_s) = rest[:6], rest[9:14]
    last, stat_bufs, rest = rest[6:9], rest[14:20], rest[20:]
    (sbuf, keep, st_a, st_m, tile, slots, small_buf, x_send, x_recv, d_send, d_recv,
     own_sem, new_sem, keep_in, keep_out, load_sem, stat_sem, n_send, n_recv, t_send, t_recv) = rest
    u_s, w_s, uu_a, ww_a, uu_m, ww_m = stat_bufs
    me, core, bits = position()
    partner = me + 1 - 2 * core
    stat_copies = [pltpu.make_async_copy(src, dst, stat_sem.at[n]) for n, (src, dst) in enumerate(zip(stats, stat_bufs))]
    for copy in stat_copies:
        copy.start()
    signal_all(me)

    def chunk(g, j):
        return (st_a, st_m)[j > 0], *chunk_columns(g, j)

    def loads(g, j):
        buf, n, cols = chunk(g, j)
        return [pltpu.make_async_copy(ref.at[:, cols], buf.at[n, k], load_sem.at[g, j, k]) for k, ref in enumerate(banks[j > 0])]

    for copy in stat_copies:
        copy.wait()
    for g, j in ORDER:
        for copy in loads(g, j):
            copy.start()

    lane = lax.broadcasted_iota(jnp.int32, (TILE, LANES), 1)
    out = jnp.zeros((TILE, LANES), F32)

    def pad8(x):
        return jnp.concatenate([x, jnp.zeros((8 - x.shape[0], x.shape[1]), F32)], axis=0)

    for k, (a, m, s) in enumerate([(uu_a, uu_m, u_s), (ww_a, ww_m, w_s)]):
        a, m, s = a[...], m[...], s[...] * s[...]
        vec = jnp.where(lax.broadcasted_iota(jnp.int32, SMALL, 1) < HALF, s, 0.0)
        wide = s - vec
        blocks = [a[:TILE], pad8(a[TILE:]), pad8(m)] + [vec[rows] for rows in BLOCKS] + [sum(wide[rows] for rows in BLOCKS)]
        for l, block in enumerate(blocks):
            out = jnp.where(lane == TILE * k + l, jnp.sum(block, axis=1, keepdims=True), out)
    tile[...] = out
    slots[me] = out
    spread(me, lambda peer: tile, slots, n_send, n_recv)
    gather_wait(me, lambda peer: tile, slots, n_send, n_recv)
    root = jnp.sqrt(sum(slots[slot] for slot in range(DEVICES)))
    ratio = [LEARN_RATE * (root[:, 8 + l:9 + l] / root[:, l:l + 1]) for l in range(8)]

    def place(g, r, j):
        owner = 2 * chip_at(bits, flips_of(g, lax.rem(r, 2), lax.rem(r // 2, 2), r // 4)) + core
        return full.at[owner, g, j]

    def landing(g, r, j, arrived):
        return last[g].at[j] if arrived is LAST else place(g, r, j)

    def keep_copies(g, j):
        return (pltpu.make_async_copy(last[g].at[j], keep.at[g, j], keep_in.at[g, j]),
                pltpu.make_async_copy(keep.at[g, j], place(g, LAST, j), keep_out.at[g, j]))

    def copy_to(g, r, j, to, arrived, sends, recvs, src, dst=None):
        return pltpu.make_async_remote_copy(
            src_ref=src, dst_ref=place(g, r, j) if dst is None else dst, send_sem=sends.at[g, arrived, j], recv_sem=recvs.at[g, arrived, j],
            device_id=(to,), device_id_type=MESH)

    def forward(g, r, j, step, src=None):
        axis = AXES[g][step]
        to = me + WEIGHT[axis] * 2 * (1 - 2 * bits[axis])
        arrived = r + WEIGHT[step]
        copy_to(g, r, j, to, arrived, x_send, x_recv, place(g, r, j) if src is None else src, landing(g, r, j, arrived)).start()

    def to_partner(g, r, j, src=None):
        return copy_to(g, r, j, partner, r, d_send, d_recv, place(g, r, j) if src is None else src)

    def arrival(g, r, j):
        return copy_to(g, r, j, partner, r, x_send, x_recv, place(g, r, j), landing(g, r, j, r))

    def own_copy(g, j):
        return pltpu.make_async_copy(sbuf.at[g, j], place(g, 0, j), own_sem.at[g, j])

    def new_copy(g, j):
        buf, n, cols = chunk(g, j)
        return pltpu.make_async_copy(buf.at[n, 0], (nw_a, nw_m)[j > 0].at[:, cols], new_sem.at[g, j])

    for g, j in ORDER:
        for copy in loads(g, j):
            copy.wait()
        buf, n, _ = chunk(g, j)
        scale = jnp.concatenate([ratio[0], ratio[1][0:4]], axis=0) if j == 0 else ratio[2][0:6]

        @pl.loop(0, STEPS)
        def _(step):
            def new(lo):
                cols = pl.ds(pl.multiple_of(lo * LANES + step * STEP, STEP), STEP)
                w, m, v = (buf[n, k, :, cols] for k in range(GROUPS))
                value = w - scale * direction(w, m, v)
                buf[n, 0, :, cols] = value
                return value

            pack_rows(j, new, lambda lo, value: put_cols(sbuf.at[g, j], lo, step, value.astype(BF16)))

        forward(g, 0, j, 0, sbuf.at[g, j])
        own_copy(g, j).start()
        new_copy(g, j).start()

    for step in (1, 2):
        for g, j in ORDER:
            forward(g, 0, j, step, sbuf.at[g, j])
    for g, j in ORDER:
        to_partner(g, 0, j, sbuf.at[g, j]).start()
    for rows, scale in zip(BLOCKS, ratio[3:]):
        nw_s[rows] = w_s[rows] - jnp.where(lane < HALF, scale, ratio[7]) * u_s[rows]
    small_buf[...] = nw_s[...].astype(BF16)
    spread(me, lambda peer: small_buf, small_full, t_send, t_recv)

    def receive(r, steps):
        for g, j in ORDER:
            arrival(g, r, j).wait_recv()
            for step in steps:
                forward(g, r, j, step)
            to_partner(g, r, j, landing(g, r, j, r)).start()
            if r is LAST:
                keep_copies(g, j)[0].start()

    receive(1, (1, 2))
    receive(2, (2,))
    receive(LAST, ())

    @pl.loop(LAST + 1, ANTIPODE)
    def _(r):
        receive(r, ())

    for g, j in ORDER:
        into, out_of = keep_copies(g, j)
        into.wait()
        out_of.start()

    gather_wait(me, lambda peer: small_buf, small_full, t_send, t_recv)
    small_full[me] = small_buf[...]
    for g, j in ORDER:
        own_copy(g, j).wait()
        keep_copies(g, j)[1].wait()
        new_copy(g, j).wait()

    @pl.loop(0, ANTIPODE)
    def _(r):
        for g, j in ORDER:
            to_partner(g, r, j).wait()

    @pl.loop(1, ANTIPODE)
    def _(r):
        for g, j in ORDER:
            arrival(g, r, j).wait_send()


def gather_call(*args):
    hbm = pl.BlockSpec(memory_space=pl.ANY)
    vmem = pl.BlockSpec(memory_space=pltpu.VMEM)
    dma = pltpu.SemaphoreType.DMA
    sems = [dma((GROUPS, TILE, PARTS))] * 4 + [dma((GROUPS, PARTS))] * 4 + [dma((GROUPS, PARTS, GROUPS)), dma((6,))] + [dma((DEVICES,))] * 4
    return pl.pallas_call(
        gather_kernel,
        out_shape=[jax.ShapeDtypeStruct((PARTS, TILE, CHUNK), BF16)] * GROUPS + [
            jax.ShapeDtypeStruct((DEVICES, GROUPS, PARTS, TILE, CHUNK), BF16),
            jax.ShapeDtypeStruct((DEVICES,) + SMALL, BF16),
            jax.ShapeDtypeStruct((A_ROWS, ATTN_W), F32),
            jax.ShapeDtypeStruct((M_ROWS, MLP_W), F32),
            jax.ShapeDtypeStruct(SMALL, F32),
        ],
        in_specs=[hbm] * len(args),
        out_specs=[hbm] * (GROUPS + 1) + [vmem, hbm, hbm, vmem],
        scratch_shapes=[pltpu.VMEM(x.shape, F32) for x in args[6:]] + [
            pltpu.VMEM((GROUPS, PARTS, TILE, CHUNK), BF16),
            pltpu.VMEM((GROUPS, PARTS, TILE, CHUNK), BF16),
            pltpu.VMEM((3, 3, A_ROWS, ATTN_COLS), F32),
            pltpu.VMEM((M_ROWS, 3, M_ROWS, MLP_COLS), F32),
            pltpu.VMEM((TILE, LANES), F32),
            pltpu.VMEM((DEVICES, TILE, LANES), F32),
            pltpu.VMEM(SMALL, BF16),
        ] + sems,
        compiler_params=pltpu.CompilerParams(collective_id=1, has_side_effects=True, vmem_limit_bytes=VMEM_LIMIT),
        name="all_gather",
    )(*args)


def unpack_moves(g, j, owner):
    if j == 0:
        start = owner * ATTN_W + g * ATTN_COLS
        moves = [(0, 8, 0, 2, 0, 0)] + [(4 * t, 4, 2, 1, 8, t) for t in range(2)]
    else:
        start = owner * MLP_W + (2 * g + j - 1) * MLP_COLS
        moves = [(0, 4, 0, 3, 0, 0), (4, 2, 0, 3, 4, 0)] + [(M_ROWS, 2, t, 1, 2 * t, 3) for t in range(GROUPS)]
    third = KT * LANES
    for row, rows, lo, width, to, at in moves:
        cols = pl.ds(pl.multiple_of(start + at * third, third), width * third)
        yield (pl.ds(row, rows), pl.ds(lo * third, width * third)), (pl.ds(to, rows), cols)


def stream(count, owner_of, source, reps, buf, load_sem, out_sem):
    def loads(t):
        slot = lax.rem(t, buf.shape[0])
        return [pltpu.make_async_copy(source(t, g, j), buf.at[slot, g, j], load_sem.at[slot, g, j]) for g, j in ORDER]

    def outs(t, g, j):
        slot = lax.rem(t, buf.shape[0])
        return [pltpu.make_async_copy(buf.at[(slot, g, j) + src], reps[j > 0].at[dst], out_sem.at[slot, g, j, n])
                for n, (src, dst) in enumerate(unpack_moves(g, j, owner_of(t)))]

    def begin(t):
        for copy in loads(t):
            copy.start()

    def move(t):
        for (g, j), copy in zip(ORDER, loads(t)):
            copy.wait()
            for out in outs(t, g, j):
                out.start()

    def drain(t):
        for g, j in ORDER:
            for out in outs(t, g, j):
                out.wait()

    begin(0)
    begin(1)
    if count > 2:
        @pl.loop(0, count)
        def _(t):
            pl.when(t >= 2)(lambda: drain(t - 2))
            pl.when(t < count - 2)(lambda: begin(t + 2))
            move(t)
    else:
        move(0)
        move(1)
    drain(count - 2)
    drain(count - 1)


def far_owner(skip):
    _, core, bits = position()
    far = 2 * chip_at(bits, (1, 1, 1))
    return lambda t: lax.rem(far + skip + t, DEVICES), far, core


def unpack_kernel(full, small_full, nw_s, rep_a, rep_m, rep_vec, rep_wide, nw_vec, nw_wide, *scratch):
    owner_of = far_owner(2)[0]
    stream(FIRST_OWNERS, owner_of, lambda t, g, j: full.at[owner_of(t), g, j], (rep_a, rep_m), *scratch)
    vec = nw_vec.shape
    nw_vec[...] = nw_s[:vec[0], :vec[1]]
    nw_wide[...] = jnp.concatenate(wide_pieces(nw_s), axis=1)
    shares = [small_full[n].astype(F32) for n in range(DEVICES)]
    rep_vec[...] = jnp.concatenate([x[:vec[0], :vec[1]] for x in shares], axis=1).astype(BF16)
    rep_wide[...] = jnp.concatenate([piece for x in shares for piece in wide_pieces(x)], axis=1).astype(BF16)


def more_kernel(full, *refs):
    owner_of = far_owner(2 + FIRST_OWNERS)[0]
    stream(DEVICES - 2 - FIRST_OWNERS, owner_of, lambda t, g, j: full.at[owner_of(t), g, j], refs[-5:-3], *refs[-3:])


def far_kernel(*refs):
    _, far, core = far_owner(0)
    stream(2, lambda t: far + flip(core, t), lambda t, g, j: refs[t * GROUPS + g].at[j], refs[-5:-3], *refs[-3:])


REPLICAS = [jax.ShapeDtypeStruct((A_ROWS, DEVICES * ATTN_W), BF16), jax.ShapeDtypeStruct((M_ROWS, DEVICES * MLP_W), BF16)]


def stream_call(kernel, name, ins, vmem_ins=(), vmem_outs=(), reps=()):
    hbm = pl.BlockSpec(memory_space=pl.ANY)
    vmem = pl.BlockSpec(memory_space=pltpu.VMEM)
    dma = pltpu.SemaphoreType.DMA
    count = len(ins) + len(vmem_ins)
    return pl.pallas_call(
        kernel,
        in_specs=[hbm] * len(ins) + [vmem] * len(vmem_ins) + [hbm] * len(reps),
        out_specs=[hbm] * 2 + [vmem] * len(vmem_outs),
        out_shape=REPLICAS + list(vmem_outs),
        scratch_shapes=[pltpu.VMEM((QUADS, GROUPS, PARTS, TILE, CHUNK), BF16), dma((QUADS, GROUPS, PARTS)), dma((QUADS, GROUPS, PARTS, 5))],
        input_output_aliases={count + n: n for n in range(len(reps))},
        cost_estimate=pl.CostEstimate(flops=10 ** 9, bytes_accessed=2 ** 26, transcendentals=0),
        compiler_params=pltpu.CompilerParams(vmem_limit_bytes=VMEM_LIMIT),
        name=name,
    )(*ins, *vmem_ins, *reps)


def swap(x, weight):
    return lax.ppermute(x, "data", [(d, d ^ weight) for d in range(DEVICES)])


def solution(mesh):
    grad_spec = P("data", None, None)
    shard_spec = P(None, "data")
    full_spec = P(None, None)

    def local_step(*banks):
        grads, weights, firsts, seconds = (banks[n:n + 4] for n in range(0, len(banks), 4))
        gs_a, gs_m, gs_s, clip = reduce_call(grads[0], grads[1], grads[3], grads[2])
        attn, mlp, wide, vec = zip(weights, firsts, seconds)
        outs = update_call((gs_a,) + attn, (gs_m,) + mlp, clip, gs_s, *vec, *wide)
        nm_a, nv_a, nm_m, nv_m, nm_vec, nv_vec, nm_wide, nv_wide = outs[:8]
        outs = gather_call(weights[0], nm_a, nv_a, weights[1], nm_m, nv_m, *outs[8:])
        last, (full, small_full, nw_a, nw_m, nw_s) = outs[:GROUPS], outs[GROUPS:]
        far = [swap(x, 2 * WEIGHT[axes[2]]) for x, axes in zip(last, AXES)]
        tail = [jax.ShapeDtypeStruct(shape, dtype) for dtype, bank in ((BF16, grads), (F32, weights)) for shape in (bank[3].shape[-2:], bank[2].shape[-2:])]
        rep_a, rep_m, rep_vec, rep_wide, nw_vec, nw_wide = stream_call(unpack_kernel, "unpack", [full], (small_full, nw_s), tail)
        far, rep_a, rep_m = lax.optimization_barrier((far, rep_a, rep_m))
        across = [swap(x, 1) for x in far]
        reps = stream_call(more_kernel, "unpack_more", [full] + far, reps=(rep_a, rep_m))
        rep_a, rep_m = stream_call(far_kernel, "unpack_far", far + across, reps=reps)
        return (rep_a, rep_m, rep_wide, rep_vec, nw_a, nw_m, nw_wide, nw_vec,
                nm_a, nm_m, nm_wide, nm_vec, nv_a, nv_m, nv_wide, nv_vec)

    return jax.shard_map(local_step, mesh=mesh, in_specs=(grad_spec,) * 4 + (shard_spec,) * 12, out_specs=(full_spec,) * 4 + (shard_spec,) * 12, check_vma=False)
```
